8 devices in a mesh: dp: 1 (over z), cp: 8 (over y, x, core).
Axes of the slice: x: 2, y: 2, z: 1, core: 2. Of those that a mesh axis runs over, the one named last changes fastest.
Arguments:
- queries: bfloat16 [512, 24, 128], P(('dp', 'cp'))
- key_new: bfloat16 [512, 8, 128], P(('dp', 'cp'))
- value_new: bfloat16 [512, 8, 128], P(('dp', 'cp'))
- key_cache: bfloat16 [12288, 8, 128], P(('dp', 'cp'))
- value_cache: bfloat16 [12288, 8, 128], P(('dp', 'cp'))
- prefix_len: int32 [1], P('dp')
Outputs:
- output 1: bfloat16 [512, 24, 128], P(('dp', 'cp'))
- output 2: float32 [512, 24], P(('dp', 'cp'))
All inputs are finite; a program needn't handle non-finite values.
Results may differ from the reference program's by a relative error of at most 0.00891405.
Values are sent between devices in bfloat16 or wider.
A program may use at most 1 GiB of HBM per device.

```python
import math
import jax
import jax.numpy as jnp
from jax import lax

GROUP_SIZE = 8
NEW_DEV = 64
PREFIX_DEV = 1536
Q_HEADS = 24
KV_HEADS = 8
HEAD_DIM = 128
NEW_LEN = GROUP_SIZE * NEW_DEV
P_MAX = GROUP_SIZE * PREFIX_DEV
GROUP_RATIO = Q_HEADS // KV_HEADS


def setup_inputs(seed: int = 0, part: int = 0) -> dict:
    base_key = jax.random.fold_in(jax.random.key(seed), part)
    rand_keys = jax.random.split(base_key, 9)
    shift_scale = GROUP_SIZE ** 0.5
    new_boost = math.log(P_MAX / NEW_LEN) * 2.0 ** 0.5
    direction = jax.random.normal(rand_keys[0], (KV_HEADS, HEAD_DIM), jnp.float32)
    direction = direction / jnp.linalg.norm(direction, axis=-1, keepdims=True)
    q_mean = jnp.repeat(direction, GROUP_RATIO, axis=0) * HEAD_DIM ** 0.5
    q_noise = jax.random.normal(rand_keys[1], (NEW_LEN, Q_HEADS, HEAD_DIM), jnp.float32)
    queries = (q_noise + q_mean[None]) * 0.5 ** 0.5
    key_new = jax.random.normal(rand_keys[2], (NEW_LEN, KV_HEADS, HEAD_DIM), jnp.float32) + new_boost * direction[None]
    new_shift = jax.random.normal(rand_keys[3], (GROUP_SIZE, 1, KV_HEADS, HEAD_DIM), jnp.float32) * shift_scale
    value_new = jax.random.normal(rand_keys[4], (GROUP_SIZE, NEW_DEV, KV_HEADS, HEAD_DIM), jnp.float32) + new_shift
    key_cache = jax.random.normal(rand_keys[5], (P_MAX, KV_HEADS, HEAD_DIM), jnp.float32)
    cache_shift = jax.random.normal(rand_keys[6], (GROUP_SIZE, 1, KV_HEADS, HEAD_DIM), jnp.float32) * shift_scale
    value_cache = jax.random.normal(rand_keys[7], (GROUP_SIZE, PREFIX_DEV, KV_HEADS, HEAD_DIM), jnp.float32) + cache_shift
    prefix_len = jax.random.randint(rand_keys[8], (1,), (3 * P_MAX) // 4, P_MAX + 1, jnp.int32)
    return {
        'queries': queries.astype(jnp.bfloat16),
        'key_new': key_new.astype(jnp.bfloat16),
        'value_new': value_new.reshape(NEW_LEN, KV_HEADS, HEAD_DIM).astype(jnp.bfloat16),
        'key_cache': key_cache.astype(jnp.bfloat16),
        'value_cache': value_cache.reshape(P_MAX, KV_HEADS, HEAD_DIM).astype(jnp.bfloat16),
        'prefix_len': prefix_len,
    }


def reference(queries, key_new, value_new, key_cache, value_cache, prefix_len):
    prefix_end = prefix_len[0]
    key_pos = jnp.arange(P_MAX + NEW_LEN)
    logit_scale = HEAD_DIM ** -0.5

    def one_head(head_idx):
        kv_idx = head_idx // GROUP_RATIO
        keys_all = jnp.concatenate([lax.dynamic_index_in_dim(key_cache, kv_idx, axis=1, keepdims=False), lax.dynamic_index_in_dim(key_new, kv_idx, axis=1, keepdims=False)], axis=0).astype(jnp.float32)
        vals_all = jnp.concatenate([lax.dynamic_index_in_dim(value_cache, kv_idx, axis=1, keepdims=False), lax.dynamic_index_in_dim(value_new, kv_idx, axis=1, keepdims=False)], axis=0).astype(jnp.float32)
        q_head = lax.dynamic_index_in_dim(queries, head_idx, axis=1, keepdims=False).astype(jnp.float32).reshape(GROUP_SIZE, NEW_DEV, HEAD_DIM)

        def one_block(block_args):
            q_rows, row_start = block_args
            scores = jnp.dot(q_rows, keys_all.T) * logit_scale
            q_pos = row_start + jnp.arange(NEW_DEV)
            visible = jnp.where(key_pos[None, :] < P_MAX, key_pos[None, :] < prefix_end, key_pos[None, :] - P_MAX <= q_pos[:, None])
            scores = jnp.where(visible, scores, -jnp.inf)
            row_max = jnp.max(scores, axis=-1)
            exp_scores = jnp.exp(scores - row_max[:, None])
            row_sum = jnp.sum(exp_scores, axis=-1)
            prob_bf = exp_scores.astype(jnp.bfloat16).astype(jnp.float32)
            block_out = jnp.dot(prob_bf, vals_all) / row_sum[:, None]
            return block_out.astype(jnp.bfloat16), row_max + jnp.log(row_sum)

        head_out, head_lse = lax.map(one_block, (q_head, jnp.arange(GROUP_SIZE) * NEW_DEV))
        return head_out.reshape(NEW_LEN, HEAD_DIM), head_lse.reshape(NEW_LEN)

    all_out, all_lse = lax.map(one_head, jnp.arange(Q_HEADS))
    return jnp.transpose(all_out, (1, 0, 2)), jnp.transpose(all_lse)
```

```python
import functools
import math

import jax
import jax.numpy as jnp
from jax import lax
from jax.experimental import pallas as pl
from jax.experimental.pallas import tpu as pltpu
from jax.sharding import PartitionSpec as P

MESH = pl.DeviceIdType.MESH
NEG = -1e30
CHIPS = 4
TOK = 64
CTOK = 2 * TOK
PRE = 1536
CPRE = 2 * PRE
HD = 128
KVH = 8
KH = KVH // 2
G = 3
QH = KH * G
KEYS = CPRE + CTOK
TILES = KH * 6
STEP = 1024
SCALE = HD ** -0.5
SCALE2 = SCALE * math.log2(math.e)
NT = (((1,), (1,)), ((), ()))
NN = (((1,), (0,)), ((), ()))
CHUNKS = [(c, STEP) for c in range(0, CPRE, STEP)] + [(CPRE, CTOK)]


def kernel(prefix_ref, q_hbm, k_hbm, vt_hbm, kn_hbm, vn_hbm, out_hbm, lse_hbm,
           q_buf, k_buf, vt_buf, vn_buf, bias_buf, fresh_buf, s_buf, max_buf,
           o_buf, l_buf, r_buf, rl_buf, fin_buf, finl_buf,
           loc_sem, kv_send, kv_recv, q_send, q_recv, p_send, p_recv, o_send, o_recv, l_send, l_recv,
           f_send, f_recv, f_loc):
    me = lax.axis_index('cp')
    core = lax.rem(me, 2)
    chip = me // 2
    other = 1 - core

    def dev(r, c):
        return {'cp': (chip ^ r) * 2 + c}

    barrier = pltpu.get_barrier_semaphore()
    for r in range(CHIPS):
        for flip in range(2):
            if r or flip:
                pl.semaphore_signal(barrier, inc=1, device_id=dev(r, core if not flip else other), device_id_type=MESH)

    def my(ref, n, c):
        return ref.at[pl.ds(c * n, n)]

    tok_at = pl.ds(core * TOK, TOK)
    pre_at = pl.ds(pl.multiple_of(core * PRE, PRE), PRE)
    new_at = pl.ds(CPRE + core * TOK, TOK)
    local = [pltpu.make_async_copy(q_hbm.at[pl.ds(core * QH, QH)], q_buf.at[0, :, tok_at], loc_sem.at[0])]
    for k in range(KH):
        h = core * KH + k
        local.append(pltpu.make_async_copy(k_hbm.at[h], k_buf.at[k, pre_at], loc_sem.at[1 + 2 * k]))
        local.append(pltpu.make_async_copy(vt_hbm.at[h], vt_buf.at[k, :, pre_at], loc_sem.at[2 + 2 * k]))
    local.append(pltpu.make_async_copy(kn_hbm.at[pl.ds(core * KH, KH)], k_buf.at[:, new_at], loc_sem.at[9]))
    local.append(pltpu.make_async_copy(vn_hbm.at[pl.ds(core * KH, KH)], vn_buf.at[:, tok_at], loc_sem.at[10]))
    for c in local:
        c.start()

    def remote(src, dst, send, recv, r, c):
        return pltpu.make_async_remote_copy(src, dst, send, recv, device_id=dev(r, c), device_id_type=MESH)

    def q_copy(r, k, flip):
        c = other if flip else core
        src = q_hbm.at[pl.ds(c * QH + k * G, G)]
        return remote(src, q_buf.at[r, pl.ds(k * G, G), tok_at], q_send.at[r, k, flip], q_recv.at[r, k, flip], r, c)

    part_q = remote(q_hbm.at[pl.ds(other * QH, QH)], q_buf.at[0, :, tok_at], p_send.at[0], p_recv.at[0], 0, other)
    part_kn = remote(kn_hbm.at[pl.ds(other * KH, KH)], k_buf.at[:, new_at], p_send.at[1], p_recv.at[1], 0, other)
    part_vn = remote(vn_hbm.at[pl.ds(other * KH, KH)], vn_buf.at[:, tok_at], p_send.at[2], p_recv.at[2], 0, other)

    def part_k(k):
        return remote(k_hbm.at[other * KH + k], k_buf.at[k, pre_at], kv_send.at[0, k], kv_recv.at[0, k], 0, other)

    def part_v(k):
        return remote(vt_hbm.at[other * KH + k], vt_buf.at[k, :, pre_at], kv_send.at[1, k], kv_recv.at[1, k], 0, other)

    pl.semaphore_wait(barrier, 2 * CHIPS - 1)
    part_q.start()
    part_kn.start()
    part_k(0).start()
    for k in range(KH):
        for r in range(1, CHIPS):
            for flip in range(2):
                q_copy(r, k, flip).start()
    part_vn.start()
    part_v(0).start()
    for k in range(1, KH):
        part_k(k).start()
        part_v(k).start()

    pos = chip * CPRE + lax.broadcasted_iota(jnp.int32, (KEYS, HD), 0)
    first = lax.broadcasted_iota(jnp.int32, (KEYS, HD), 1) == 0
    hidden = (pos >= prefix_ref[0]) & (lax.broadcasted_iota(jnp.int32, (KEYS, HD), 0) < CPRE)
    bias_buf[...] = jnp.where(first & hidden, NEG, 0.0).astype(jnp.bfloat16)
    key_id = chip * CTOK + lax.broadcasted_iota(jnp.int32, (CTOK, CTOK), 0)
    for r in range(CHIPS):
        q_id = (chip ^ r) * CTOK + lax.broadcasted_iota(jnp.int32, (CTOK, CTOK), 1)
        fresh_buf[r] = jnp.where(key_id <= q_id, 0.0, NEG)

    for c in local:
        c.wait()
    part_q.wait_recv()
    part_kn.wait_recv()
    part_vn.wait_recv()
    for k in range(KH):
        vt_buf[k, :, CPRE:] = vn_buf[k].T

    ones = (lax.broadcasted_iota(jnp.int32, (2 * CTOK, HD), 1) == 0).astype(jnp.bfloat16)

    def q_tile(t):
        k = t // 6
        g = lax.rem(t, 6) // 2
        h = lax.rem(t, 2)
        q = jnp.concatenate([q_buf[2 * h, k * G + g], q_buf[2 * h + 1, k * G + g]], axis=0)
        return k, h, jnp.concatenate([q, ones], axis=1)

    def scores(k, h, q, c, n, top):
        keys = jnp.concatenate([k_buf[k, pl.ds(c, n), :], bias_buf[pl.ds(c, n), :]], axis=1)
        s = lax.dot_general(keys, q, NT, preferred_element_type=jnp.float32)
        if c == CPRE:
            s = s + jnp.concatenate([fresh_buf[2 * h], fresh_buf[2 * h + 1]], axis=1)
        s_buf[pl.ds(c, n), :] = s
        part = s.reshape(n // 16, 16, 2 * CTOK).max(axis=0)
        return part if top is None else jnp.maximum(top, part)

    def values(k, c, n, ref_pt, total, acc):
        p = jnp.exp2(s_buf[pl.ds(c, n), :] * SCALE2 - ref_pt)
        part = p.reshape(n // 16, 16, 2 * CTOK).sum(axis=0)
        total = part if total is None else total + part
        d = lax.dot_general(vt_buf[k, :, pl.ds(c, n)], p.astype(jnp.bfloat16), NN, preferred_element_type=jnp.float32)
        return total, (d if acc is None else acc + d)

    def set_max(top):
        max_buf[...] = jnp.broadcast_to(top.max(axis=0, keepdims=True), (8, 2 * CTOK))

    def wait_for(t):
        k = t // 6

        @pl.when(lax.rem(t, 6) == 0)
        def _():
            part_k(k).wait_recv()
            part_v(k).wait_recv()
            for flip in range(2):
                q_copy(1, k, flip).wait_recv()

        @pl.when(lax.rem(t, 6) == 1)
        def _():
            for r in (2, 3):
                for flip in range(2):
                    q_copy(r, k, flip).wait_recv()

    def o_copy(r, k):
        rows = pl.ds(k * G, G)
        return remote(o_buf.at[r, rows], r_buf.at[r - 1, rows], o_send.at[r - 1, k], o_recv.at[r - 1, k], r, core)

    def l_copy(r, k):
        return remote(l_buf.at[r, k], rl_buf.at[r - 1, k], l_send.at[r - 1, k], l_recv.at[r - 1, k], r, core)

    wait_for(0)
    k, h, q = q_tile(0)
    top = None
    for c, n in CHUNKS:
        top = scores(k, h, q, c, n, top)
    set_max(top)

    @pl.loop(0, TILES)
    def _(t):
        nxt = jnp.minimum(t + 1, TILES - 1)

        @pl.when(t < TILES - 1)
        def _():
            wait_for(t + 1)

        k = t // 6
        g = lax.rem(t, 6) // 2
        h = lax.rem(t, 2)
        k2, h2, q2 = q_tile(nxt)
        raw = max_buf[0:1]
        ref_pt = raw * SCALE2
        top = total = acc = None
        for c, n in CHUNKS:
            total, acc = values(k, c, n, ref_pt, total, acc)
            top = scores(k2, h2, q2, c, n, top)
        set_max(top)
        total = total.sum(axis=0, keepdims=True)
        o = (acc / total).astype(jnp.bfloat16)
        lse = raw * SCALE + jnp.log(total)
        for i in range(2):
            o_buf[2 * h + i, k * G + g] = o[:, i * CTOK:(i + 1) * CTOK]
            l_buf[2 * h + i, k, pl.ds(g, 1), :] = lse[:, i * CTOK:(i + 1) * CTOK]

        @pl.when(lax.rem(t, 6) == 5)
        def _():
            for r in (3, 1, 2):
                o_copy(r, k).start()
                l_copy(r, k).start()

    @pl.loop(0, KH)
    def _(k):
        for r in range(1, CHIPS):
            o_copy(r, k).wait_recv()
            l_copy(r, k).wait_recv()
        for g in range(G):
            ls = [l_buf[0, k, g:g + 1, :]] + [rl_buf[r, k, g:g + 1, :] for r in range(3)]
            top = jnp.maximum(jnp.maximum(ls[0], ls[1]), jnp.maximum(ls[2], ls[3]))
            ws = [jnp.exp(l - top) for l in ls]
            z = (ws[0] + ws[1]) + (ws[2] + ws[3])
            finl_buf[0, k, g:g + 1, :] = top + jnp.log(z)
            os = [o_buf[0, k * G + g]] + [r_buf[r, k * G + g] for r in range(3)]
            o = sum((w / z) * x.astype(jnp.float32) for w, x in zip(ws, os))
            fin_buf[k * G + g] = o.T.astype(jnp.bfloat16)

    mine = pltpu.make_async_copy(fin_buf.at[:, tok_at], out_hbm.at[pl.ds(core * QH, QH)], f_loc.at[0])
    their_at = pl.ds(other * TOK, TOK)
    theirs = remote(fin_buf.at[:, their_at], out_hbm.at[pl.ds(core * QH, QH)], f_send.at[0], f_recv.at[0], 0, other)
    mine_l = pltpu.make_async_copy(finl_buf.at[0], lse_hbm.at[core], f_loc.at[1])
    theirs_l = remote(finl_buf.at[0], lse_hbm.at[core], f_send.at[1], f_recv.at[1], 0, other)
    for c in (theirs, theirs_l, mine, mine_l):
        c.start()

    part_q.wait_send()
    part_kn.wait_send()
    part_vn.wait_send()

    @pl.loop(0, KH)
    def _(k):
        part_k(k).wait_send()
        part_v(k).wait_send()
        for r in range(1, CHIPS):
            for flip in range(2):
                q_copy(r, k, flip).wait_send()
            o_copy(r, k).wait_send()
            l_copy(r, k).wait_send()

    for c in (theirs, theirs_l, mine, mine_l):
        c.wait()


def solution(mesh):
    tok_spec = P(('dp', 'cp'))
    bf, f32 = jnp.bfloat16, jnp.float32
    dma = pltpu.SemaphoreType.DMA

    def local_attend(queries, key_new, value_new, key_cache, value_cache, prefix_len):
        core = lax.rem(lax.axis_index('cp'), 2)
        any_spec = pl.BlockSpec(memory_space=pl.ANY)
        out, lse = pl.pallas_call(
            kernel,
            out_shape=(jax.ShapeDtypeStruct((2 * QH, TOK, HD), bf), jax.ShapeDtypeStruct((2, KH, 8, CTOK), f32)),
            in_specs=[pl.BlockSpec(memory_space=pltpu.SMEM)] + [any_spec] * 5,
            out_specs=(any_spec, any_spec),
            scratch_shapes=[
                pltpu.VMEM((CHIPS, QH, CTOK, HD), bf),
                pltpu.VMEM((KH, KEYS, HD), bf),
                pltpu.VMEM((KH, HD, KEYS), bf),
                pltpu.VMEM((KH, CTOK, HD), bf),
                pltpu.VMEM((KEYS, HD), bf),
                pltpu.VMEM((CHIPS, CTOK, CTOK), f32),
                pltpu.VMEM((KEYS, 2 * CTOK), f32),
                pltpu.VMEM((8, 2 * CTOK), f32),
                pltpu.VMEM((CHIPS, QH, HD, CTOK), bf),
                pltpu.VMEM((CHIPS, KH, 8, CTOK), f32),
                pltpu.VMEM((3, QH, HD, CTOK), bf),
                pltpu.VMEM((3, KH, 8, CTOK), f32),
                pltpu.VMEM((QH, CTOK, HD), bf),
                pltpu.VMEM((1, KH, 8, CTOK), f32),
                dma((11,)), dma((2, KH)), dma((2, KH)), dma((CHIPS, KH, 2)), dma((CHIPS, KH, 2)), dma((3,)), dma((3,)),
                dma((3, KH)), dma((3, KH)), dma((3, KH)), dma((3, KH)), dma((2,)), dma((2,)), dma((2,)),
            ],
            compiler_params=pltpu.CompilerParams(
                collective_id=0, has_side_effects=True, vmem_limit_bytes=48 << 20),
        )(prefix_len, queries.transpose(1, 0, 2), key_cache.transpose(1, 0, 2), value_cache.transpose(1, 2, 0),
          key_new.transpose(1, 0, 2), value_new.transpose(1, 0, 2))
        attn_out = out.transpose(1, 0, 2)
        lse = lse[:, :, :G].reshape(2 * QH, CTOK)
        row_lse = lax.dynamic_slice(lse, (0, core * TOK), (2 * QH, TOK)).T
        return attn_out, row_lse

    return jax.shard_map(local_attend, mesh=mesh, in_specs=(tok_spec, tok_spec, tok_spec, tok_spec, tok_spec, P('dp')),
                         out_specs=(tok_spec, tok_spec), check_vma=False)
```

```python
import math

import jax
import jax.numpy as jnp
from jax import lax
from jax.experimental import pallas as pl
from jax.experimental.pallas import tpu as pltpu
from jax.sharding import PartitionSpec as P

MESH = pl.DeviceIdType.MESH
NEG = -1e30
CHIPS = 4
TOK = 64
CTOK = 2 * TOK
PRE = 1536
CPRE = 2 * PRE
HD = 128
HALF = HD // 2
KVH = 8
KH = KVH // 2
G = 3
QH = KH * G
KEYS = CPRE + CTOK
TILES = KH * 6
STEP = 1024
BLK = 128
SCALE = HD ** -0.5
SCALE2 = SCALE * math.log2(math.e)
NT = (((1,), (1,)), ((), ()))
NN = (((1,), (0,)), ((), ()))
CHUNKS = [(c, STEP) for c in range(0, CPRE, STEP)] + [(CPRE, CTOK)]
LOADS = 4


def kernel(prefix_ref, q_hbm, k_hbm, v_hbm, kn_hbm, vn_hbm, out_hbm, lse_hbm,
           q_raw, k_raw, v_raw, kn_raw, vn_raw, qt_buf, ks_buf, vs_buf, kns_buf, vns_buf,
           q_buf, k_buf, vt_buf, vn_buf, bias_buf, fresh_buf, s_buf, max_buf,
           o_buf, l_buf, t_buf, tl_buf, r_buf, rl_buf, fin_buf, finl_buf,
           in_sem, kv_send, kv_recv, n_send, n_recv, q_send, q_recv, p_send, p_recv, d_send, d_recv,
           t_send, t_recv, tl_send, tl_recv, o_send, o_recv, l_send, l_recv, f_send, f_recv, f_loc, fl_sem):
    me = lax.axis_index('cp')
    core = lax.rem(me, 2)
    chip = me // 2
    other = 1 - core

    def dev(r, c):
        return {'cp': (chip ^ r) * 2 + c}

    def remote(src, dst, send, recv, r, c):
        return pltpu.make_async_remote_copy(src, dst, send, recv, device_id=dev(r, c), device_id_type=MESH)

    part = PRE // LOADS
    loads = [pltpu.make_async_copy(q_hbm, q_raw, in_sem.at[0]),
             pltpu.make_async_copy(kn_hbm, kn_raw, in_sem.at[1]),
             pltpu.make_async_copy(vn_hbm, vn_raw, in_sem.at[2])]
    k_loads = [pltpu.make_async_copy(k_hbm.at[pl.ds(i * part, part)], k_raw.at[pl.ds(i * part, part)], in_sem.at[3 + i])
               for i in range(LOADS)]
    v_loads = [pltpu.make_async_copy(v_hbm.at[pl.ds(i * part, part)], v_raw.at[pl.ds(i * part, part)], in_sem.at[3 + LOADS + i])
               for i in range(LOADS)]
    for c in loads + k_loads + v_loads:
        c.start()

    barrier = pltpu.get_barrier_semaphore()
    peers = [dev(1, 0), dev(1, 1), dev(2, 0), dev(2, 1), dev(0, other)]
    for peer in peers:
        pl.semaphore_signal(barrier, inc=1, device_id=peer, device_id_type=MESH)

    tok_at = pl.ds(core * TOK, TOK)
    pre_at = pl.ds(pl.multiple_of(core * PRE, PRE), PRE)
    new_at = pl.ds(CPRE + core * TOK, TOK)

    def q_copy(r, k, plane):
        rows = pl.ds(k * G, G)
        return remote(qt_buf.at[pl.ds(plane * QH + k * G, G)], q_buf.at[r, rows, tok_at],
                      q_send.at[r - 1, k, plane], q_recv.at[r - 1, k, core], r, plane)

    def q_wait(r, k, s):
        rows = pl.ds(k * G, G)
        remote(qt_buf.at[rows], q_buf.at[r, rows, pl.ds(s * TOK, TOK)],
               q_send.at[r - 1, k, s], q_recv.at[r - 1, k, s], r, s).wait_recv()

    def send_q(k):
        for plane in range(2):
            for r in (1, 2):
                q_copy(r, k, plane).start()

    def hop(i, k):
        rows, half = pl.ds(k * G, G), pl.ds(i * TOK, TOK)
        return remote(q_buf.at[1 + i, rows, half], q_buf.at[3, rows, half], d_send.at[i, k], d_recv.at[i, k], 2 - i, core)

    def forward(k):
        for r in (1, 2):
            for s in range(2):
                q_wait(r, k, s)
        for i in range(2):
            hop(i, k).start()

    def diagonal(k):
        for i in range(2):
            hop(i, k).wait_recv()

    part_q = remote(qt_buf.at[pl.ds(other * QH, QH)], q_buf.at[0, :, tok_at], p_send.at[0], p_recv.at[0], 0, other)
    part_kn = remote(kns_buf, k_buf.at[:, new_at], n_send.at[0], n_recv.at[0], 0, other)
    part_vn = remote(vns_buf, vn_buf.at[:, tok_at], n_send.at[1], n_recv.at[1], 0, other)

    def part_k(k):
        return remote(ks_buf.at[k], k_buf.at[k, pre_at], kv_send.at[0, k], kv_recv.at[0, k], 0, other)

    def part_v(k):
        return remote(vs_buf.at[k], vt_buf.at[k, :, pre_at], kv_send.at[1, k], kv_recv.at[1, k], 0, other)

    loads[0].wait()
    y = jnp.swapaxes(q_raw[...], 0, 1)
    qt_buf[...] = y
    for c in range(2):
        @pl.when(core == c)
        def _():
            q_buf[0, :, c * TOK:(c + 1) * TOK, :] = qt_buf[c * QH:(c + 1) * QH]
    pl.semaphore_wait(barrier, len(peers))
    send_q(0)
    part_q.start()
    send_q(1)

    loads[1].wait()
    for c in range(2):
        @pl.when(core == c)
        def _():
            y = jnp.swapaxes(kn_raw[...], 0, 1)
            k_buf[:, CPRE + c * TOK:CPRE + (c + 1) * TOK, :] = y[c * KH:(c + 1) * KH]
            kns_buf[...] = y[(1 - c) * KH:(2 - c) * KH]
    part_kn.start()
    for i in range(LOADS):
        k_loads[i].wait()
        for c in range(2):
            @pl.when(core == c)
            def _():
                @pl.loop(i * part // BLK, (i + 1) * part // BLK)
                def _(b):
                    at = pl.multiple_of(b * BLK, BLK)
                    y = jnp.swapaxes(k_raw[pl.ds(at, BLK)], 0, 1)
                    k_buf[:, pl.ds(c * PRE + at, BLK), :] = y[c * KH:(c + 1) * KH]
                    ks_buf[:, pl.ds(at, BLK), :] = y[(1 - c) * KH:(2 - c) * KH]
    for k in range(KH):
        part_k(k).start()

    loads[2].wait()
    for c in range(2):
        @pl.when(core == c)
        def _():
            y = jnp.swapaxes(vn_raw[...], 0, 1)
            vn_buf[:, c * TOK:(c + 1) * TOK, :] = y[c * KH:(c + 1) * KH]
            vns_buf[...] = y[(1 - c) * KH:(2 - c) * KH]
    part_vn.start()
    for i in range(LOADS):
        v_loads[i].wait()
        for c in range(2):
            @pl.when(core == c)
            def _():
                @pl.loop(i * part // BLK, (i + 1) * part // BLK)
                def _(b):
                    at = pl.multiple_of(b * BLK, BLK)
                    y = jnp.swapaxes(v_raw[pl.ds(at, BLK)], 0, 1)
                    for k in range(KH):
                        vt_buf[k, :, pl.ds(c * PRE + at, BLK)] = y[c * KH + k].T
                        vs_buf[k, :, pl.ds(at, BLK)] = y[(1 - c) * KH + k].T
    for k in range(KH):
        part_v(k).start()

    row = lax.broadcasted_iota(jnp.int32, (KEYS, HD), 0)
    first = lax.broadcasted_iota(jnp.int32, (KEYS, HD), 1) == 0
    hidden = (chip * CPRE + row >= prefix_ref[0]) & (row < CPRE)
    bias_buf[...] = jnp.where(first & hidden, NEG, 0.0).astype(jnp.bfloat16)
    key_id = chip * CTOK + lax.broadcasted_iota(jnp.int32, (CTOK, CTOK), 0)
    for r in range(CHIPS):
        q_id = (chip ^ r) * CTOK + lax.broadcasted_iota(jnp.int32, (CTOK, CTOK), 1)
        fresh_buf[r] = jnp.where(key_id <= q_id, 0.0, NEG)

    ones = (lax.broadcasted_iota(jnp.int32, (2 * CTOK, HD), 1) == 0).astype(jnp.bfloat16)

    def groups(t):
        k = t // 6
        z = (k + 2) // 4
        out = []
        for i in range(2):
            at = 2 * lax.rem(t, 6) + i
            seg = at // 3
            out.append((seg + z * (3 - 2 * seg), k * G + lax.rem(at, 3), lax.rem(at, 3)))
        return k, out

    def q_tile(t):
        k, gs = groups(t)
        q = jnp.concatenate([q_buf[r, head] for r, head, _ in gs], axis=0)
        return k, gs, jnp.concatenate([q, ones], axis=1)

    def scores(k, gs, q, c, n, top):
        keys = jnp.concatenate([k_buf[k, pl.ds(c, n), :], bias_buf[pl.ds(c, n), :]], axis=1)
        s = lax.dot_general(keys, q, NT, preferred_element_type=jnp.float32)
        if c == CPRE:
            s = s + jnp.concatenate([fresh_buf[r] for r, _, _ in gs], axis=1)
        s_buf[pl.ds(c, n), :] = s
        up = s.reshape(n // 16, 16, 2 * CTOK).max(axis=0)
        return up if top is None else jnp.maximum(top, up)

    def values(k, c, n, ref_pt, total, acc):
        p = jnp.exp2(s_buf[pl.ds(c, n), :] * SCALE2 - ref_pt)
        up = p.reshape(n // 16, 16, 2 * CTOK).sum(axis=0)
        total = up if total is None else total + up
        d = lax.dot_general(vt_buf[k, :, pl.ds(c, n)], p.astype(jnp.bfloat16), NN, preferred_element_type=jnp.float32)
        return total, (d if acc is None else acc + d)

    def set_max(top):
        max_buf[...] = jnp.broadcast_to(top.max(axis=0, keepdims=True), (8, 2 * CTOK))

    def to_near(i, k):
        rows = pl.ds(k * G, G)
        return (remote(o_buf.at[3, rows, pl.ds(i * HALF, HALF)], t_buf.at[i, rows], t_send.at[i, k], t_recv.at[i, k], 1 + i, core),
                remote(l_buf.at[3, k], tl_buf.at[i, k], tl_send.at[i, k], tl_recv.at[i, k], 1 + i, core))

    def to_home(r, k):
        rows = pl.ds(k * G, G)
        return (remote(o_buf.at[r, rows], r_buf.at[r - 1, rows], o_send.at[r - 1, k], o_recv.at[r - 1, k], r, core),
                remote(l_buf.at[r, k], rl_buf.at[r - 1, k], l_send.at[r - 1, k], l_recv.at[r - 1, k], r, core))

    def give_diagonal(k):
        for i in range(2):
            for c in to_near(i, k):
                c.start()

    def join(k):
        for i in range(2):
            r = 2 - i
            for c in to_near(i, k):
                c.wait_recv()
            la, lb = l_buf[r, k, 0:G, :], tl_buf[i, k, 0:G, :]
            top = jnp.maximum(la, lb)
            wa, wb = jnp.exp(la - top), jnp.exp(lb - top)
            z = wa + wb
            l_buf[r, k, G:2 * G, :] = top + jnp.log(z)
            wa, wb = wa / z, wb / z
            for g in range(G):
                at = pl.ds(i * HALF, HALF)
                o = (wa[g:g + 1] * o_buf[r, k * G + g, at, :].astype(jnp.float32)
                     + wb[g:g + 1] * t_buf[i, k * G + g].astype(jnp.float32))
                o_buf[r, k * G + g, at, :] = o.astype(jnp.bfloat16)
            for c in to_home(r, k):
                c.start()

    part_q.wait_recv()
    part_kn.wait_recv()
    part_k(0).wait_recv()
    k, gs, q = q_tile(0)
    top = None
    for c, n in CHUNKS:
        top = scores(k, gs, q, c, n, top)
    set_max(top)
    part_vn.wait_recv()
    for k in range(KH):
        vt_buf[k, :, CPRE:] = vn_buf[k].T
    part_v(0).wait_recv()
    forward(0)
    send_q(2)

    def serve(t, at, fn, *args):
        @pl.when(t == at)
        def _():
            for a in args:
                fn(a)

    def cache_of(k):
        part_k(k).wait_recv()
        part_v(k).wait_recv()

    @pl.loop(0, TILES)
    def _(t):
        k, gs = groups(t)
        k2, gs2, q2 = q_tile(jnp.minimum(t + 1, TILES - 1))
        raw = max_buf[0:1]
        ref_pt = raw * SCALE2
        top = total = acc = None
        for c, n in CHUNKS:
            total, acc = values(k, c, n, ref_pt, total, acc)
            top = scores(k2, gs2, q2, c, n, top)
        set_max(top)
        total = total.sum(axis=0, keepdims=True)
        o = (acc / total).astype(jnp.bfloat16)
        lse = raw * SCALE + jnp.log(total)
        for i, (r, head, g) in enumerate(gs):
            o_buf[r, head] = o[:, i * CTOK:(i + 1) * CTOK]
            l_buf[r, k, pl.ds(g, 1), :] = lse[:, i * CTOK:(i + 1) * CTOK]

        serve(t, 2, forward, 1)
        serve(t, 2, send_q, 3)
        serve(t, 2, diagonal, 0)
        serve(t, 4, cache_of, 1)
        serve(t, 5, forward, 2)
        serve(t, 5, give_diagonal, 0)
        serve(t, 8, join, 0)
        serve(t, 8, diagonal, 1)
        serve(t, 9, forward, 3)
        serve(t, 10, cache_of, 2)
        serve(t, 10, diagonal, 2)
        serve(t, 11, give_diagonal, 1)
        serve(t, 13, give_diagonal, 2)
        serve(t, 14, join, 1)
        serve(t, 16, join, 2)
        serve(t, 16, cache_of, 3)
        serve(t, 16, diagonal, 3)
        serve(t, 19, give_diagonal, 3)
        serve(t, 22, join, 3)

    their_at = pl.ds(other * TOK, TOK)

    def out_copies(k):
        rows = pl.ds(k * G, G)
        dst = out_hbm.at[pl.ds(core * QH + k * G, G)]
        return (pltpu.make_async_copy(fin_buf.at[rows, tok_at], dst, f_loc.at[k]),
                remote(fin_buf.at[rows, their_at], dst, f_send.at[k], f_recv.at[k], 0, other))

    @pl.loop(0, KH)
    def _(k):
        for r in (1, 2):
            for c in to_home(r, k):
                c.wait_recv()
        own = l_buf[0, k, 0:G, :]
        ls = [[own, rl_buf[0, k, 0:G, :], rl_buf[1, k, G:2 * G, :]],
              [own, rl_buf[0, k, G:2 * G, :], rl_buf[1, k, 0:G, :]]]
        weights = []
        for half in range(2):
            top = jnp.maximum(jnp.maximum(ls[half][0], ls[half][1]), ls[half][2])
            ws = [jnp.exp(l - top) for l in ls[half]]
            z = ws[0] + ws[1] + ws[2]
            if half == 0:
                finl_buf[k, 0:G, :] = top + jnp.log(z)
            weights.append([w / z for w in ws])
        for g in range(G):
            head = k * G + g
            halves = []
            for half in range(2):
                at = pl.ds(half * HALF, HALF)
                xs = [o_buf[0, head, at, :], r_buf[0, head, at, :], r_buf[1, head, at, :]]
                halves.append(sum(w[g:g + 1] * x.astype(jnp.float32) for w, x in zip(weights[half], xs)))
            fin_buf[head] = jnp.concatenate(halves, axis=0).T.astype(jnp.bfloat16)
        for c in reversed(out_copies(k)):
            c.start()

    mine_l = pltpu.make_async_copy(finl_buf, lse_hbm.at[core], fl_sem.at[0])
    theirs_l = remote(finl_buf, lse_hbm.at[core], fl_sem.at[1], fl_sem.at[2], 0, other)
    theirs_l.start()
    mine_l.start()

    part_q.wait_send()
    part_kn.wait_send()
    part_vn.wait_send()

    @pl.loop(0, KH)
    def _(k):
        part_k(k).wait_send()
        part_v(k).wait_send()
        for r in (1, 2):
            for plane in range(2):
                q_copy(r, k, plane).wait_send()
            for c in to_home(r, k):
                c.wait_send()
        for i in range(2):
            hop(i, k).wait_send()
            for c in to_near(i, k):
                c.wait_send()
        for c in out_copies(k):
            c.wait()

    theirs_l.wait()
    mine_l.wait()


def solution(mesh):
    tok_spec = P(('dp', 'cp'))
    bf, f32 = jnp.bfloat16, jnp.float32
    dma = pltpu.SemaphoreType.DMA

    def local_attend(queries, key_new, value_new, key_cache, value_cache, prefix_len):
        core = lax.rem(lax.axis_index('cp'), 2)
        any_spec = pl.BlockSpec(memory_space=pl.ANY)
        out, lse = pl.pallas_call(
            kernel,
            out_shape=(jax.ShapeDtypeStruct((2 * QH, TOK, HD), bf), jax.ShapeDtypeStruct((2, KH, 8, CTOK), f32)),
            in_specs=[pl.BlockSpec(memory_space=pltpu.SMEM)] + [any_spec] * 5,
            out_specs=(any_spec, any_spec),
            scratch_shapes=[
                pltpu.VMEM((TOK, 2 * QH, HD), bf),
                pltpu.VMEM((PRE, KVH, HD), bf),
                pltpu.VMEM((PRE, KVH, HD), bf),
                pltpu.VMEM((TOK, KVH, HD), bf),
                pltpu.VMEM((TOK, KVH, HD), bf),
                pltpu.VMEM((2 * QH, TOK, HD), bf),
                pltpu.VMEM((KH, PRE, HD), bf),
                pltpu.VMEM((KH, HD, PRE), bf),
                pltpu.VMEM((KH, TOK, HD), bf),
                pltpu.VMEM((KH, TOK, HD), bf),
                pltpu.VMEM((CHIPS, QH, CTOK, HD), bf),
                pltpu.VMEM((KH, KEYS, HD), bf),
                pltpu.VMEM((KH, HD, KEYS), bf),
                pltpu.VMEM((KH, CTOK, HD), bf),
                pltpu.VMEM((KEYS, HD), bf),
                pltpu.VMEM((CHIPS, CTOK, CTOK), f32),
                pltpu.VMEM((KEYS, 2 * CTOK), f32),
                pltpu.VMEM((8, 2 * CTOK), f32),
                pltpu.VMEM((CHIPS, QH, HD, CTOK), bf),
                pltpu.VMEM((CHIPS, KH, 8, CTOK), f32),
                pltpu.VMEM((2, QH, HALF, CTOK), bf),
                pltpu.VMEM((2, KH, 8, CTOK), f32),
                pltpu.VMEM((2, QH, HD, CTOK), bf),
                pltpu.VMEM((2, KH, 8, CTOK), f32),
                pltpu.VMEM((QH, CTOK, HD), bf),
                pltpu.VMEM((KH, 8, CTOK), f32),
                dma((3 + 2 * LOADS,)),
                dma((2, KH)), dma((2, KH)),
                dma((2,)), dma((2,)),
                dma((2, KH, 2)), dma((2, KH, 2)),
                dma((1,)), dma((1,)),
                dma((2, KH)), dma((2, KH)),
                dma((2, KH)), dma((2, KH)),
                dma((2, KH)), dma((2, KH)),
                dma((2, KH)), dma((2, KH)),
                dma((2, KH)), dma((2, KH)),
                dma((KH,)), dma((KH,)), dma((KH,)),
                dma((3,)),
            ],
            compiler_params=pltpu.CompilerParams(
                collective_id=0, has_side_effects=True, vmem_limit_bytes=48 << 20),
        )(prefix_len, queries, key_cache, value_cache, key_new, value_new)
        attn_out = out.transpose(1, 0, 2)
        lse = lse[:, :, :G].reshape(2 * QH, CTOK)
        row_lse = lax.dynamic_slice(lse, (0, core * TOK), (2 * QH, TOK)).T
        return attn_out, row_lse

    return jax.shard_map(local_attend, mesh=mesh, in_specs=(tok_spec, tok_spec, tok_spec, tok_spec, tok_spec, P('dp')),
                         out_specs=(tok_spec, tok_spec), check_vma=False)
```

```python
import math

import jax
import jax.numpy as jnp
from jax import lax
from jax.experimental import pallas as pl
from jax.experimental.pallas import tpu as pltpu
from jax.sharding import PartitionSpec as P

MESH = pl.DeviceIdType.MESH
NEG = -1e30
CHIPS = 4
TOK = 64
CTOK = 2 * TOK
PRE = 1536
CPRE = 2 * PRE
HD = 128
HALF = HD // 2
KVH = 8
KH = KVH // 2
G = 3
QH = KH * G
KEYS = CPRE + CTOK
TILES = KH * 6
STEP = 1024
BLK = 128
SCALE = HD ** -0.5
SCALE2 = SCALE * math.log2(math.e)
NT = (((1,), (1,)), ((), ()))
NN = (((1,), (0,)), ((), ()))
CHUNKS = [(c, STEP) for c in range(0, CPRE, STEP)] + [(CPRE, CTOK)]
LOADS = 4


def kernel(prefix_ref, q_hbm, k_hbm, v_hbm, kn_hbm, vn_hbm, out_hbm, lse_hbm,
           q_raw, k_raw, v_raw, kn_raw, vn_raw, qt_buf, ks_buf, vs_buf, kns_buf, vns_buf,
           q_buf, k_buf, vt_buf, vn_buf, bias_buf, fresh_buf, s_buf, max_buf,
           o_buf, l_buf, t_buf, tl_buf, r_buf, rl_buf, fin_buf, finl_buf,
           in_sem, kv_send, kv_recv, n_send, n_recv, q_send, q_recv, p_send, p_recv, d_send, d_recv,
           t_send, t_recv, tl_send, tl_recv, o_send, o_recv, l_send, l_recv, f_send, f_recv, f_loc, fl_sem):
    me = lax.axis_index('cp')
    core = lax.rem(me, 2)
    chip = me // 2
    other = 1 - core

    def dev(r, c):
        return {'cp': (chip ^ r) * 2 + c}

    def remote(src, dst, send, recv, r, c):
        return pltpu.make_async_remote_copy(src, dst, send, recv, device_id=dev(r, c), device_id_type=MESH)

    part = PRE // LOADS
    loads = [pltpu.make_async_copy(q_hbm, q_raw, in_sem.at[0]),
             pltpu.make_async_copy(kn_hbm, kn_raw, in_sem.at[1]),
             pltpu.make_async_copy(vn_hbm, vn_raw, in_sem.at[2])]
    k_loads = [pltpu.make_async_copy(k_hbm.at[pl.ds(i * part, part)], k_raw.at[pl.ds(i * part, part)], in_sem.at[3 + i])
               for i in range(LOADS)]
    v_loads = [pltpu.make_async_copy(v_hbm.at[pl.ds(i * part, part)], v_raw.at[pl.ds(i * part, part)], in_sem.at[3 + LOADS + i])
               for i in range(LOADS)]
    for c in loads + k_loads + v_loads:
        c.start()

    barrier = pltpu.get_barrier_semaphore()
    peers = [dev(1, 0), dev(1, 1), dev(2, 0), dev(2, 1), dev(0, other)]
    for peer in peers:
        pl.semaphore_signal(barrier, inc=1, device_id=peer, device_id_type=MESH)

    tok_at = pl.ds(core * TOK, TOK)
    pre_at = pl.ds(pl.multiple_of(core * PRE, PRE), PRE)
    new_at = pl.ds(CPRE + core * TOK, TOK)

    def q_copy(r, k, plane):
        rows = pl.ds(k * G, G)
        return remote(qt_buf.at[pl.ds(plane * QH + k * G, G)], q_buf.at[r, rows, tok_at],
                      q_send.at[r - 1, k, plane], q_recv.at[r - 1, k, core], r, plane)

    def q_wait(r, k, s):
        rows = pl.ds(k * G, G)
        remote(qt_buf.at[rows], q_buf.at[r, rows, pl.ds(s * TOK, TOK)],
               q_send.at[r - 1, k, s], q_recv.at[r - 1, k, s], r, s).wait_recv()

    def send_q(k):
        for plane in range(2):
            for r in (1, 2):
                q_copy(r, k, plane).start()

    def hop(i, k):
        rows, half = pl.ds(k * G, G), pl.ds(i * TOK, TOK)
        return remote(q_buf.at[1 + i, rows, half], q_buf.at[3, rows, half], d_send.at[i, k], d_recv.at[i, k], 2 - i, core)

    def forward(k):
        for r in (1, 2):
            for s in range(2):
                q_wait(r, k, s)
        for i in range(2):
            hop(i, k).start()

    def diagonal(k):
        for i in range(2):
            hop(i, k).wait_recv()

    part_q = remote(qt_buf.at[pl.ds(other * QH, QH)], q_buf.at[0, :, tok_at], p_send.at[0], p_recv.at[0], 0, other)
    part_kn = remote(kns_buf, k_buf.at[:, new_at], n_send.at[0], n_recv.at[0], 0, other)
    part_vn = remote(vns_buf, vn_buf.at[:, tok_at], n_send.at[1], n_recv.at[1], 0, other)

    def part_k(k):
        return remote(ks_buf.at[k], k_buf.at[k, pre_at], kv_send.at[0, k], kv_recv.at[0, k], 0, other)

    def part_v(k):
        return remote(vs_buf.at[k], vt_buf.at[k, :, pre_at], kv_send.at[1, k], kv_recv.at[1, k], 0, other)

    loads[0].wait()
    y = jnp.swapaxes(q_raw[...], 0, 1)
    qt_buf[...] = y
    for c in range(2):
        @pl.when(core == c)
        def _():
            q_buf[0, :, c * TOK:(c + 1) * TOK, :] = qt_buf[c * QH:(c + 1) * QH]
    pl.semaphore_wait(barrier, len(peers))
    send_q(0)
    part_q.start()
    send_q(1)

    loads[1].wait()
    for c in range(2):
        @pl.when(core == c)
        def _():
            y = jnp.swapaxes(kn_raw[...], 0, 1)
            k_buf[:, CPRE + c * TOK:CPRE + (c + 1) * TOK, :] = y[c * KH:(c + 1) * KH]
            kns_buf[...] = y[(1 - c) * KH:(2 - c) * KH]
    part_kn.start()
    for i in range(LOADS):
        k_loads[i].wait()
        for c in range(2):
            @pl.when(core == c)
            def _():
                @pl.loop(i * part // BLK, (i + 1) * part // BLK)
                def _(b):
                    at = pl.multiple_of(b * BLK, BLK)
                    y = jnp.swapaxes(k_raw[pl.ds(at, BLK)], 0, 1)
                    k_buf[:, pl.ds(c * PRE + at, BLK), :] = y[c * KH:(c + 1) * KH]
                    ks_buf[:, pl.ds(at, BLK), :] = y[(1 - c) * KH:(2 - c) * KH]
    for k in range(KH):
        part_k(k).start()

    loads[2].wait()
    for c in range(2):
        @pl.when(core == c)
        def _():
            y = jnp.swapaxes(vn_raw[...], 0, 1)
            vn_buf[:, c * TOK:(c + 1) * TOK, :] = y[c * KH:(c + 1) * KH]
            vns_buf[...] = y[(1 - c) * KH:(2 - c) * KH]
    part_vn.start()
    for i in range(LOADS):
        v_loads[i].wait()
        for c in range(2):
            @pl.when(core == c)
            def _():
                @pl.loop(i * part // BLK, (i + 1) * part // BLK)
                def _(b):
                    at = pl.multiple_of(b * BLK, BLK)
                    y = jnp.swapaxes(v_raw[pl.ds(at, BLK)], 0, 1)
                    for k in range(KH):
                        vt_buf[k, :, pl.ds(c * PRE + at, BLK)] = y[c * KH + k].T
                        vs_buf[k, :, pl.ds(at, BLK)] = y[(1 - c) * KH + k].T
    for k in range(KH):
        part_v(k).start()

    row = lax.broadcasted_iota(jnp.int32, (KEYS, HD), 0)
    first = lax.broadcasted_iota(jnp.int32, (KEYS, HD), 1) == 0
    hidden = (chip * CPRE + row >= prefix_ref[0]) & (row < CPRE)
    bias_buf[...] = jnp.where(first & hidden, NEG, 0.0).astype(jnp.bfloat16)
    key_id = chip * CTOK + lax.broadcasted_iota(jnp.int32, (CTOK, CTOK), 0)
    for r in range(CHIPS):
        q_id = (chip ^ r) * CTOK + lax.broadcasted_iota(jnp.int32, (CTOK, CTOK), 1)
        fresh_buf[r] = jnp.where(key_id <= q_id, 0.0, NEG)

    ones = (lax.broadcasted_iota(jnp.int32, (2 * CTOK, HD), 1) == 0).astype(jnp.bfloat16)

    def groups(t):
        k = t // 6
        z = (k + 2) // 4
        out = []
        for i in range(2):
            at = 2 * lax.rem(t, 6) + i
            seg = at // 3
            out.append((seg + z * (3 - 2 * seg), k * G + lax.rem(at, 3), lax.rem(at, 3)))
        return k, out

    def q_tile(t):
        k, gs = groups(t)
        q = jnp.concatenate([q_buf[r, head] for r, head, _ in gs], axis=0)
        return k, gs, jnp.concatenate([q, ones], axis=1)

    def scores(k, gs, q, c, n, top):
        keys = jnp.concatenate([k_buf[k, pl.ds(c, n), :], bias_buf[pl.ds(c, n), :]], axis=1)
        s = lax.dot_general(keys, q, NT, preferred_element_type=jnp.float32)
        if c == CPRE:
            s = s + jnp.concatenate([fresh_buf[r] for r, _, _ in gs], axis=1)
        s_buf[pl.ds(c, n), :] = s
        up = s.reshape(n // 16, 16, 2 * CTOK).max(axis=0)
        return up if top is None else jnp.maximum(top, up)

    def values(k, c, n, ref_pt, total, acc):
        p = jnp.exp2(s_buf[pl.ds(c, n), :] * SCALE2 - ref_pt)
        up = p.reshape(n // 16, 16, 2 * CTOK).sum(axis=0)
        total = up if total is None else total + up
        d = lax.dot_general(vt_buf[k, :, pl.ds(c, n)], p.astype(jnp.bfloat16), NN, preferred_element_type=jnp.float32)
        return total, (d if acc is None else acc + d)

    def set_max(top):
        max_buf[...] = jnp.broadcast_to(top.max(axis=0, keepdims=True), (8, 2 * CTOK))

    def to_near(i, k):
        rows = pl.ds(k * G, G)
        return (remote(o_buf.at[3, rows, pl.ds(i * HALF, HALF)], t_buf.at[i, rows], t_send.at[i, k], t_recv.at[i, k], 1 + i, core),
                remote(l_buf.at[3, k], tl_buf.at[i, k], tl_send.at[i, k], tl_recv.at[i, k], 1 + i, core))

    def to_home(r, k):
        rows = pl.ds(k * G, G)
        return (remote(o_buf.at[r, rows], r_buf.at[r - 1, rows], o_send.at[r - 1, k], o_recv.at[r - 1, k], r, core),
                remote(l_buf.at[r, k], rl_buf.at[r - 1, k], l_send.at[r - 1, k], l_recv.at[r - 1, k], r, core))

    def give_diagonal(k):
        for i in range(2):
            for c in to_near(i, k):
                c.start()

    def join(k):
        for i in range(2):
            r = 2 - i
            for c in to_near(i, k):
                c.wait_recv()
            la, lb = l_buf[r, k, 0:G, :], tl_buf[i, k, 0:G, :]
            top = jnp.maximum(la, lb)
            wa, wb = jnp.exp(la - top), jnp.exp(lb - top)
            z = wa + wb
            l_buf[r, k, G:2 * G, :] = top + jnp.log(z)
            wa, wb = wa / z, wb / z
            for g in range(G):
                at = pl.ds(i * HALF, HALF)
                o = (wa[g:g + 1] * o_buf[r, k * G + g, at, :].astype(jnp.float32)
                     + wb[g:g + 1] * t_buf[i, k * G + g].astype(jnp.float32))
                o_buf[r, k * G + g, at, :] = o.astype(jnp.bfloat16)
            for c in to_home(r, k):
                c.start()

    part_q.wait_recv()
    part_kn.wait_recv()
    part_k(0).wait_recv()
    k, gs, q = q_tile(0)
    top = None
    for c, n in CHUNKS:
        top = scores(k, gs, q, c, n, top)
    set_max(top)
    part_vn.wait_recv()
    for k in range(KH):
        vt_buf[k, :, CPRE:] = vn_buf[k].T
    part_v(0).wait_recv()
    forward(0)
    send_q(2)

    def serve(t, at, fn, *args):
        @pl.when(t == at)
        def _():
            for a in args:
                fn(a)

    def cache_of(k):
        part_k(k).wait_recv()
        part_v(k).wait_recv()

    @pl.loop(0, TILES)
    def _(t):
        k, gs = groups(t)
        k2, gs2, q2 = q_tile(jnp.minimum(t + 1, TILES - 1))
        raw = max_buf[0:1]
        ref_pt = raw * SCALE2
        top = total = acc = None
        for c, n in CHUNKS:
            total, acc = values(k, c, n, ref_pt, total, acc)
            top = scores(k2, gs2, q2, c, n, top)
        set_max(top)
        total = total.sum(axis=0, keepdims=True)
        o = (acc / total).astype(jnp.bfloat16)
        lse = raw * SCALE + jnp.log(total)
        for i, (r, head, g) in enumerate(gs):
            o_buf[r, head] = o[:, i * CTOK:(i + 1) * CTOK]
            l_buf[r, k, pl.ds(g, 1), :] = lse[:, i * CTOK:(i + 1) * CTOK]

        serve(t, 2, forward, 1)
        serve(t, 2, send_q, 3)
        serve(t, 2, diagonal, 0)
        serve(t, 4, cache_of, 1)
        serve(t, 5, forward, 2)
        serve(t, 5, give_diagonal, 0)
        serve(t, 8, join, 0)
        serve(t, 8, diagonal, 1)
        serve(t, 9, forward, 3)
        serve(t, 10, cache_of, 2)
        serve(t, 10, diagonal, 2)
        serve(t, 11, give_diagonal, 1)
        serve(t, 13, give_diagonal, 2)
        serve(t, 14, join, 1)
        serve(t, 16, join, 2)
        serve(t, 16, cache_of, 3)
        serve(t, 16, diagonal, 3)
        serve(t, 19, give_diagonal, 3)
        serve(t, 22, join, 3)

    their_at = pl.ds(other * TOK, TOK)

    def out_copies(k):
        rows = pl.ds(k * G, G)
        dst = out_hbm.at[pl.ds(core * QH + k * G, G)]
        return (pltpu.make_async_copy(fin_buf.at[rows, tok_at], dst, f_loc.at[k]),
                remote(fin_buf.at[rows, their_at], dst, f_send.at[k], f_recv.at[k], 0, other))

    @pl.loop(0, KH)
    def _(k):
        for r in (1, 2):
            for c in to_home(r, k):
                c.wait_recv()
        own = l_buf[0, k, 0:G, :]
        ls = [[own, rl_buf[0, k, 0:G, :], rl_buf[1, k, G:2 * G, :]],
              [own, rl_buf[0, k, G:2 * G, :], rl_buf[1, k, 0:G, :]]]
        weights = []
        for half in range(2):
            top = jnp.maximum(jnp.maximum(ls[half][0], ls[half][1]), ls[half][2])
            ws = [jnp.exp(l - top) for l in ls[half]]
            z = ws[0] + ws[1] + ws[2]
            if half == 0:
                finl_buf[k, 0:G, :] = top + jnp.log(z)
            weights.append([w / z for w in ws])
        for g in range(G):
            head = k * G + g
            halves = []
            for half in range(2):
                at = pl.ds(half * HALF, HALF)
                xs = [o_buf[0, head, at, :], r_buf[0, head, at, :], r_buf[1, head, at, :]]
                halves.append(sum(w[g:g + 1] * x.astype(jnp.float32) for w, x in zip(weights[half], xs)))
            fin_buf[head] = jnp.concatenate(halves, axis=0).T.astype(jnp.bfloat16)
        for c in reversed(out_copies(k)):
            c.start()

    mine_l = pltpu.make_async_copy(finl_buf, lse_hbm.at[core], fl_sem.at[0])
    theirs_l = remote(finl_buf, lse_hbm.at[core], fl_sem.at[1], fl_sem.at[2], 0, other)
    theirs_l.start()
    mine_l.start()

    part_q.wait_send()
    part_kn.wait_send()
    part_vn.wait_send()

    @pl.loop(0, KH)
    def _(k):
        part_k(k).wait_send()
        part_v(k).wait_send()
        for r in (1, 2):
            for plane in range(2):
                q_copy(r, k, plane).wait_send()
            for c in to_home(r, k):
                c.wait_send()
        for i in range(2):
            hop(i, k).wait_send()
            for c in to_near(i, k):
                c.wait_send()
        for c in out_copies(k):
            c.wait()

    theirs_l.wait()
    mine_l.wait()


def solution(mesh):
    tok_spec = P(('dp', 'cp'))
    bf, f32 = jnp.bfloat16, jnp.float32
    dma = pltpu.SemaphoreType.DMA

    def local_attend(queries, key_new, value_new, key_cache, value_cache, prefix_len):
        core = lax.rem(lax.axis_index('cp'), 2)
        any_spec = pl.BlockSpec(memory_space=pl.ANY)
        out, lse = pl.pallas_call(
            kernel,
            out_shape=(jax.ShapeDtypeStruct((2 * QH, TOK, HD), bf), jax.ShapeDtypeStruct((2, KH, 8, CTOK), f32)),
            in_specs=[pl.BlockSpec(memory_space=pltpu.SMEM)] + [any_spec] * 5,
            out_specs=(any_spec, any_spec),
            scratch_shapes=[
                pltpu.VMEM((TOK, 2 * QH, HD), bf),
                pltpu.VMEM((PRE, KVH, HD), bf),
                pltpu.VMEM((PRE, KVH, HD), bf),
                pltpu.VMEM((TOK, KVH, HD), bf),
                pltpu.VMEM((TOK, KVH, HD), bf),
                pltpu.VMEM((2 * QH, TOK, HD), bf),
                pltpu.VMEM((KH, PRE, HD), bf),
                pltpu.VMEM((KH, HD, PRE), bf),
                pltpu.VMEM((KH, TOK, HD), bf),
                pltpu.VMEM((KH, TOK, HD), bf),
                pltpu.VMEM((CHIPS, QH, CTOK, HD), bf),
                pltpu.VMEM((KH, KEYS, HD), bf),
                pltpu.VMEM((KH, HD, KEYS), bf),
                pltpu.VMEM((KH, CTOK, HD), bf),
                pltpu.VMEM((KEYS, HD), bf),
                pltpu.VMEM((CHIPS, CTOK, CTOK), f32),
                pltpu.VMEM((KEYS, 2 * CTOK), f32),
                pltpu.VMEM((8, 2 * CTOK), f32),
                pltpu.VMEM((CHIPS, QH, HD, CTOK), bf),
                pltpu.VMEM((CHIPS, KH, 8, CTOK), f32),
                pltpu.VMEM((2, QH, HALF, CTOK), bf),
                pltpu.VMEM((2, KH, 8, CTOK), f32),
                pltpu.VMEM((2, QH, HD, CTOK), bf),
                pltpu.VMEM((2, KH, 8, CTOK), f32),
                pltpu.VMEM((QH, CTOK, HD), bf),
                pltpu.VMEM((KH, 8, CTOK), f32),
                dma((3 + 2 * LOADS,)),
                dma((2, KH)), dma((2, KH)),
                dma((2,)), dma((2,)),
                dma((2, KH, 2)), dma((2, KH, 2)),
                dma((1,)), dma((1,)),
                dma((2, KH)), dma((2, KH)),
                dma((2, KH)), dma((2, KH)),
                dma((2, KH)), dma((2, KH)),
                dma((2, KH)), dma((2, KH)),
                dma((2, KH)), dma((2, KH)),
                dma((KH,)), dma((KH,)), dma((KH,)),
                dma((3,)),
            ],
            compiler_params=pltpu.CompilerParams(
                collective_id=0, has_side_effects=True, vmem_limit_bytes=63 << 20),
        )(prefix_len, queries, key_cache, value_cache, key_new, value_new)
        attn_out = out.transpose(1, 0, 2)
        lse = lse[:, :, :G].reshape(2 * QH, CTOK)
        row_lse = lax.dynamic_slice(lse, (0, core * TOK), (2 * QH, TOK)).T
        return attn_out, row_lse

    return jax.shard_map(local_attend, mesh=mesh, in_specs=(tok_spec, tok_spec, tok_spec, tok_spec, tok_spec, P('dp')),
                         out_specs=(tok_spec, tok_spec), check_vma=False)
```

```python
import math

import jax
import jax.numpy as jnp
from jax import lax
from jax.experimental import pallas as pl
from jax.experimental.pallas import tpu as pltpu
from jax.sharding import PartitionSpec as P

MESH = pl.DeviceIdType.MESH
NEG = -1e30
CHIPS = 4
TOK = 64
CTOK = 2 * TOK
PRE = 1536
CPRE = 2 * PRE
HD = 128
HALF = HD // 2
KVH = 8
KH = KVH // 2
G = 3
QH = KH * G
KEYS = CPRE + CTOK
TILES = KH * 6
STEP = 256
AHEAD = 14
LEAD = 4
BLK = 32
VBLK = 128
SCALE = HD ** -0.5
SCALE2 = SCALE * math.log2(math.e)
NT = (((1,), (1,)), ((), ()))
NN = (((1,), (0,)), ((), ()))
CHUNKS = [(c, STEP) for c in range(0, CPRE, STEP)] + [(CPRE, CTOK)]
LOADS = 4


def packed(digits, bits):
    return sum(d << (bits * i) for i, d in enumerate(digits))


PAIRS = [((0, 5), (1, 5)), ((0, 3), (0, 4)), ((0, 2), (1, 3)), ((1, 4), (1, 2)), ((0, 1), (0, 0)), ((1, 1), (1, 0)),
         ((2, 0), (2, 1)), ((3, 0), (3, 1)), ((2, 2), (2, 3)), ((3, 2), (3, 3)), ((2, 4), (3, 4)), ((2, 5), (3, 5))]
ORDER = [(packed([p[b][0] for p in PAIRS], 2), packed([p[b][1] % 4 for p in PAIRS], 2), packed([p[b][1] // 4 for p in PAIRS], 1))
         for b in range(2)]


def kernel(prefix_ref, q_hbm, k_hbm, v_hbm, kn_hbm, vn_hbm, out_ref, lse_ref,
           q_raw, k_raw, v_raw, kn_raw, vn_raw, qt_buf, ks_buf, vs_buf, kns_buf, vns_buf,
           q_buf, k_buf, vt_buf, vn_buf, bias_buf, fresh_buf, s0_buf, s1_buf, max_buf, top_buf, qt2_buf,
           o_buf, l_buf, t_buf, tl_buf, r_buf, rl_buf, fin_buf, finl_buf,
           in_sem, kv_send, kv_recv, n_send, n_recv, q_send, q_recv, p_send, p_recv, d_send, d_recv,
           t_send, t_recv, tl_send, tl_recv, o_send, o_recv, l_send, l_recv, f_send, f_recv, fl_sem):
    s_bufs = (s0_buf, s1_buf)
    me = lax.axis_index('cp')
    core = lax.rem(me, 2)
    chip = me // 2
    other = 1 - core

    def dev(r, c):
        return {'cp': (chip ^ r) * 2 + c}

    def remote(src, dst, send, recv, r, c):
        return pltpu.make_async_remote_copy(src, dst, send, recv, device_id=dev(r, c), device_id_type=MESH)

    part = PRE // LOADS
    loads = [pltpu.make_async_copy(q_hbm, q_raw, in_sem.at[0]),
             pltpu.make_async_copy(kn_hbm, kn_raw, in_sem.at[1]),
             pltpu.make_async_copy(vn_hbm, vn_raw, in_sem.at[2])]
    k_loads = [pltpu.make_async_copy(k_hbm.at[pl.ds(i * part, part)], k_raw.at[pl.ds(i * part, part)], in_sem.at[3 + i])
               for i in range(LOADS)]
    v_loads = [pltpu.make_async_copy(v_hbm.at[pl.ds(i * part, part)], v_raw.at[pl.ds(i * part, part)], in_sem.at[3 + LOADS + i])
               for i in range(LOADS)]
    for c in loads + k_loads + v_loads:
        c.start()

    barrier = pltpu.get_barrier_semaphore()
    peers = [dev(1, 0), dev(1, 1), dev(2, 0), dev(2, 1), dev(0, other)]
    for peer in peers:
        pl.semaphore_signal(barrier, inc=1, device_id=peer, device_id_type=MESH)

    tok_at = pl.ds(core * TOK, TOK)
    new_at = pl.ds(CPRE + core * TOK, TOK)

    def slot(r, k):
        return pl.ds(4 * G * k + G * (CHIPS - 1 - r), G)

    def q_copy(r, k, plane):
        return remote(qt_buf.at[pl.ds(plane * QH + k * G, G)], q_buf.at[slot(r, k), tok_at],
                      q_send.at[r - 1, k, plane], q_recv.at[r - 1, k, core], r, plane)

    def q_wait(r, k, s):
        remote(qt_buf.at[pl.ds(0, G)], q_buf.at[slot(r, k), pl.ds(s * TOK, TOK)],
               q_send.at[r - 1, k, s], q_recv.at[r - 1, k, s], r, s).wait_recv()

    def send_q(k):
        for plane in range(2):
            for r in (1, 2):
                q_copy(r, k, plane).start()

    def hop(i, k):
        half = pl.ds(i * TOK, TOK)
        return remote(q_buf.at[slot(1 + i, k), half], q_buf.at[slot(3, k), half], d_send.at[i, k], d_recv.at[i, k], 2 - i, core)

    def forward(k):
        for r in (1, 2):
            for s in range(2):
                q_wait(r, k, s)
        for i in range(2):
            hop(i, k).start()

    def diagonal(k):
        for i in range(2):
            hop(i, k).wait_recv()

    def part_q(k):
        return remote(qt_buf.at[pl.ds(other * QH + k * G, G)], q_buf.at[slot(0, k), tok_at], p_send.at[k], p_recv.at[k], 0, other)

    part_kn = remote(kns_buf, k_buf.at[:, new_at], n_send.at[0], n_recv.at[0], 0, other)
    part_vn = remote(vns_buf, vn_buf.at[:, tok_at], n_send.at[1], n_recv.at[1], 0, other)

    def part_k(i, two):
        heads, at = pl.ds(2 * two, 2), pl.ds(i * part, part)
        dst = pl.ds(pl.multiple_of(core * PRE + i * part, part), part)
        return remote(ks_buf.at[heads, at], k_buf.at[heads, dst], kv_send.at[0, i, two], kv_recv.at[0, i, two], 0, other)

    def part_v(i, two):
        heads, at = pl.ds(2 * two, 2), pl.ds(i * part, part)
        dst = pl.ds(pl.multiple_of(core * PRE + i * part, part), part)
        return remote(vs_buf.at[heads, :, at], vt_buf.at[heads, :, dst], kv_send.at[1, i, two], kv_recv.at[1, i, two], 0, other)

    loads[0].wait()

    @pl.loop(0, TOK // 16)
    def _(b):
        at = pl.ds(pl.multiple_of(b * 16, 16), 16)
        qt_buf[:, at, :] = jnp.swapaxes(q_raw[at], 0, 1)

    pl.semaphore_wait(barrier, len(peers))
    send_q(0)
    for k in range(KH):
        part_q(k).start()
    send_q(1)
    for c in range(2):
        @pl.when(core == c)
        def _():
            for k in range(KH):
                q_buf[slot(0, k), c * TOK:(c + 1) * TOK, :] = qt_buf[c * QH + k * G:c * QH + (k + 1) * G]

    loads[1].wait()
    for c in range(2):
        @pl.when(core == c)
        def _():
            y = jnp.swapaxes(kn_raw[...], 0, 1)
            k_buf[:, CPRE + c * TOK:CPRE + (c + 1) * TOK, :] = y[c * KH:(c + 1) * KH]
            kns_buf[...] = y[(1 - c) * KH:(2 - c) * KH]
    part_kn.start()
    for i in range(LOADS):
        k_loads[i].wait()
        for c in range(2):
            @pl.when(core == c)
            def _():
                @pl.loop(i * part // BLK, (i + 1) * part // BLK)
                def _(b):
                    at = pl.multiple_of(b * BLK, BLK)
                    y = jnp.swapaxes(k_raw[pl.ds(at, BLK)], 0, 1)
                    k_buf[:, pl.ds(c * PRE + at, BLK), :] = y[c * KH:(c + 1) * KH]
                    ks_buf[:, pl.ds(at, BLK), :] = y[(1 - c) * KH:(2 - c) * KH]
        part_k(i, 0).start()

    loads[2].wait()
    for c in range(2):
        @pl.when(core == c)
        def _():
            y = jnp.swapaxes(vn_raw[...], 0, 1)
            vn_buf[:, c * TOK:(c + 1) * TOK, :] = y[c * KH:(c + 1) * KH]
            vns_buf[...] = y[(1 - c) * KH:(2 - c) * KH]
    part_vn.start()
    for i in range(LOADS):
        v_loads[i].wait()
        for c in range(2):
            @pl.when(core == c)
            def _():
                @pl.loop(i * part // VBLK, (i + 1) * part // VBLK)
                def _(b):
                    at = pl.multiple_of(b * VBLK, VBLK)
                    y = jnp.swapaxes(v_raw[pl.ds(at, VBLK)], 0, 1)
                    for k in range(KH):
                        vt_buf[k, :, pl.ds(c * PRE + at, VBLK)] = y[c * KH + k].T
                        vs_buf[k, :, pl.ds(at, VBLK)] = y[(1 - c) * KH + k].T
        part_v(i, 0).start()

    for i in range(LOADS):
        part_k(i, 1).start()
        part_v(i, 1).start()

    row = lax.broadcasted_iota(jnp.int32, (CTOK, HD), 0)
    place = row - (lax.broadcasted_iota(jnp.int32, (CTOK, HD), 1) << 20)
    seen = prefix_ref[0] - chip * CPRE

    @pl.loop(0, CPRE // CTOK)
    def _(b):
        at = pl.multiple_of(b * CTOK, CTOK)
        bias_buf[pl.ds(at, CTOK), :] = jnp.where(place >= seen - at, NEG, 0.0).astype(jnp.bfloat16)

    bias_buf[CPRE:, :] = jnp.zeros((CTOK, HD), jnp.bfloat16)
    key_id = chip * CTOK + row
    for r in range(CHIPS):
        q_id = (chip ^ r) * CTOK + lax.broadcasted_iota(jnp.int32, (CTOK, CTOK), 1)
        mask = jnp.where(key_id <= q_id, 0.0, NEG)
        for g in range(G):
            fresh_buf[slot(r, 0).start + g] = mask

    for b in range(2):
        qt2_buf[b, :, HD:] = (lax.broadcasted_iota(jnp.int32, (2 * CTOK, HD), 1) == 0).astype(jnp.bfloat16)

    def place_of(p, b):
        kv, low, high = ORDER[b]
        k = (kv >> (2 * p)) & 3
        j = ((low >> (2 * p)) & 3) + 4 * ((high >> p) & 1)
        return k, 4 * G * k + 2 * j, 2 * j

    def load_q(n, b):
        for i in range(2):
            qt2_buf[b, i * CTOK:(i + 1) * CTOK, :HD] = q_buf[n + i]

    def fold(x, op):
        return op(x.reshape(x.shape[0] // 8, 8, 2 * CTOK), axis=0)

    def scores(k, f, b, c, top):
        at, n = CHUNKS[c]
        keys = jnp.concatenate([k_buf[k, pl.ds(at, n), :], bias_buf[pl.ds(at, n), :]], axis=1)
        s = lax.dot_general(keys, qt2_buf[b], NT, preferred_element_type=jnp.float32)
        if at == CPRE:
            s = s + jnp.concatenate([fresh_buf[f + i] for i in range(2)], axis=1)
        s_bufs[b][pl.ds(at, n), :] = s
        up = fold(s, jnp.max)
        return up if top is None else jnp.maximum(top, up)

    def values(k, b, c, ref_pt, total, acc):
        at, n = CHUNKS[c]
        p = jnp.exp2(s_bufs[b][pl.ds(at, n), :] * SCALE2 - ref_pt)
        up = fold(p, jnp.sum)
        total = up if total is None else total + up
        d = lax.dot_general(vt_buf[k, :, pl.ds(at, n)], p.astype(jnp.bfloat16), NN, preferred_element_type=jnp.float32)
        return total, (d if acc is None else acc + d)

    def advance(places, step, top):
        ahead, c = divmod(step, len(CHUNKS))
        (k, n, f), b = places[ahead], ahead % 2
        if c == 0:
            load_q(n, b)
            top = None
        top = scores(k, f, b, c, top)
        if c == len(CHUNKS) - 1:
            max_buf[b] = jnp.broadcast_to(top.max(axis=0, keepdims=True), (8, 2 * CTOK))
        return top

    def to_near(i, k):
        rows = pl.ds(k * G, G)
        return (remote(o_buf.at[slot(3, k), pl.ds(i * HALF, HALF)], t_buf.at[i, rows], t_send.at[i, k], t_recv.at[i, k], 1 + i, core),
                remote(l_buf.at[slot(3, k)], tl_buf.at[i, rows], tl_send.at[i, k], tl_recv.at[i, k], 1 + i, core))

    def to_home(r, k, g):
        n, h = pl.ds(slot(r, k).start + g, 1), pl.ds(k * G + g, 1)
        return (remote(o_buf.at[n], r_buf.at[r - 1, h], o_send.at[r - 1, k, g], o_recv.at[r - 1, k, g], r, core),
                remote(l_buf.at[n], rl_buf.at[r - 1, h], l_send.at[r - 1, k, g], l_recv.at[r - 1, k, g], r, core))

    def give_diagonal(k):
        for i in range(2):
            for c in to_near(i, k):
                c.start()

    def join(r, k, *gs):
        i = 2 - r
        if 0 in gs:
            for c in to_near(i, k):
                c.wait_recv()
        for g in gs:
            n, h, at = slot(r, k).start + g, k * G + g, pl.ds(i * HALF, HALF)
            la, lb = l_buf[n, 0:1, :], tl_buf[i, h, 0:1, :]
            top = jnp.maximum(la, lb)
            wa, wb = jnp.exp(la - top), jnp.exp(lb - top)
            z = wa + wb
            l_buf[n, 1:2, :] = top + jnp.log(z)
            o = (wa / z) * o_buf[n, at, :].astype(jnp.float32) + (wb / z) * t_buf[i, h].astype(jnp.float32)
            o_buf[n, at, :] = o.astype(jnp.bfloat16)
            for c in to_home(r, k, g):
                c.start()

    def rest_of_cache():
        for i in range(LOADS):
            part_k(i, 1).wait_recv()
            part_v(i, 1).wait_recv()

    def serve(p, at, *calls):
        @pl.when(p == at)
        def _():
            for fn, *args in calls:
                fn(*args)

    for k in range(KH):
        part_q(k).wait_recv()
    part_kn.wait_recv()
    for i in range(LOADS):
        part_k(i, 0).wait_recv()
    places = tuple(place_of(i // 2, i % 2) for i in range(4))
    top = None
    for step in range(AHEAD):
        top = advance(places, step, top)
    top_buf[...] = top
    part_vn.wait_recv()
    for k in range(KH):
        vt_buf[k, :, CPRE:] = vn_buf[k].T
    for i in range(LOADS):
        part_v(i, 0).wait_recv()
    forward(0)
    send_q(2)

    def pair(p, places):
        top = top_buf[...]
        step = AHEAD
        for _ in range(LEAD):
            top = advance(places, step, top)
            step += 1
        for b in range(2):
            k, n, _ = places[b]
            raw = max_buf[b, 0:1]
            ref_pt = raw * SCALE2
            total = acc = None
            for c in range(len(CHUNKS)):
                if step < AHEAD + 2 * len(CHUNKS):
                    top = advance(places, step, top)
                    step += 1
                total, acc = values(k, b, c, ref_pt, total, acc)
            total = total.sum(axis=0, keepdims=True)
            o = (acc / total).astype(jnp.bfloat16)
            lse = raw * SCALE + jnp.log(total)
            for i in range(2):
                o_buf[n + i] = o[:, i * CTOK:(i + 1) * CTOK]
                l_buf[n + i, 0:1, :] = lse[:, i * CTOK:(i + 1) * CTOK]
        top_buf[...] = top

        serve(p, 0, (forward, 1), (send_q, 3))
        serve(p, 2, (forward, 2), (diagonal, 0))
        serve(p, 3, (diagonal, 1), (rest_of_cache,))
        serve(p, 4, (forward, 3), (give_diagonal, 0), (diagonal, 2))
        serve(p, 5, (give_diagonal, 1), (diagonal, 3))
        serve(p, 6, (give_diagonal, 2), (join, 2, 0, 0, 1, 2), (join, 1, 0, 0, 1, 2))
        serve(p, 7, (give_diagonal, 3), (join, 2, 1, 0, 1, 2), (join, 1, 1, 0, 1, 2))
        serve(p, 8, (join, 2, 2, 0, 1, 2), (join, 1, 2, 0, 1))
        serve(p, 9, (join, 2, 3, 0, 1, 2), (join, 1, 3, 0, 1))
        serve(p, 10, (join, 1, 2, 2), (join, 1, 3, 2))
        after = jnp.minimum(p + 2, TILES // 2 - 1)
        return places[2], places[3], place_of(after, 0), place_of(after, 1)

    lax.fori_loop(0, TILES // 2, pair, places)

    their_at = pl.ds(other * TOK, TOK)

    def out_copy(k):
        rows = pl.ds(k * G, G)
        return remote(fin_buf.at[rows, their_at], out_ref.at[pl.ds(core * QH + k * G, G)], f_send.at[k], f_recv.at[k], 0, other)

    @pl.loop(0, KH)
    def _(k):
        for g in range(G):
            for r in (1, 2):
                for c in to_home(r, k, g):
                    c.wait_recv()
            n, h = slot(0, k).start + g, k * G + g
            own, near = l_buf[n, 0:1, :], [(rl_buf[i, h, 0:1, :], rl_buf[i, h, 1:2, :]) for i in range(2)]
            halves = []
            for half in range(2):
                ls = [own, near[0][half], near[1][1 - half]]
                top = jnp.maximum(jnp.maximum(ls[0], ls[1]), ls[2])
                ws = [jnp.exp(l - top) for l in ls]
                z = ws[0] + ws[1] + ws[2]
                if half == 0:
                    finl_buf[k, g:g + 1, :] = top + jnp.log(z)
                at = pl.ds(half * HALF, HALF)
                xs = [o_buf[n, at, :], r_buf[0, h, at, :], r_buf[1, h, at, :]]
                halves.append(sum((w / z) * x.astype(jnp.float32) for w, x in zip(ws, xs)))
            fin_buf[h] = jnp.concatenate(halves, axis=0).T.astype(jnp.bfloat16)
        out_copy(k).start()
        for g in range(G):
            out_ref[core * QH + k * G + g] = fin_buf[k * G + g, pl.ds(pl.multiple_of(core * TOK, TOK), TOK), :]

    theirs_l = remote(finl_buf, lse_ref.at[core], fl_sem.at[0], fl_sem.at[1], 0, other)
    theirs_l.start()
    lse_ref[core] = finl_buf[...]

    part_kn.wait_send()
    part_vn.wait_send()

    @pl.loop(0, KH)
    def _(k):
        part_q(k).wait_send()
        for two in range(2):
            part_k(k, two).wait_send()
            part_v(k, two).wait_send()
        for r in (1, 2):
            for plane in range(2):
                q_copy(r, k, plane).wait_send()
            for g in range(G):
                for c in to_home(r, k, g):
                    c.wait_send()
        for i in range(2):
            hop(i, k).wait_send()
            for c in to_near(i, k):
                c.wait_send()
        out_copy(k).wait()

    theirs_l.wait()


def solution(mesh):
    tok_spec = P(('dp', 'cp'))
    bf, f32 = jnp.bfloat16, jnp.float32
    dma = pltpu.SemaphoreType.DMA

    def local_attend(queries, key_new, value_new, key_cache, value_cache, prefix_len):
        core = lax.rem(lax.axis_index('cp'), 2)
        hbm = pl.BlockSpec(memory_space=pltpu.HBM)
        vmem = pl.BlockSpec(memory_space=pltpu.VMEM)
        out, lse = pl.pallas_call(
            kernel,
            out_shape=(pltpu.VMEM((2 * QH, TOK, HD), bf), pltpu.VMEM((2, KH, 8, CTOK), f32)),
            in_specs=[pl.BlockSpec(memory_space=pltpu.SMEM)] + [hbm] * 5,
            out_specs=(vmem, vmem),
            scratch_shapes=[
                pltpu.VMEM((TOK, 2 * QH, HD), bf),
                pltpu.VMEM((PRE, KVH, HD), bf),
                pltpu.VMEM((PRE, KVH, HD), bf),
                pltpu.VMEM((TOK, KVH, HD), bf),
                pltpu.VMEM((TOK, KVH, HD), bf),
                pltpu.VMEM((2 * QH, TOK, HD), bf),
                pltpu.VMEM((KH, PRE, HD), bf),
                pltpu.VMEM((KH, HD, PRE), bf),
                pltpu.VMEM((KH, TOK, HD), bf),
                pltpu.VMEM((KH, TOK, HD), bf),
                pltpu.VMEM((CHIPS * QH, CTOK, HD), bf),
                pltpu.VMEM((KH, KEYS, HD), bf),
                pltpu.VMEM((KH, HD, KEYS), bf),
                pltpu.VMEM((KH, CTOK, HD), bf),
                pltpu.VMEM((KEYS, HD), bf),
                pltpu.VMEM((CHIPS * G, CTOK, CTOK), f32),
                pltpu.VMEM((KEYS, 2 * CTOK), f32),
                pltpu.VMEM((KEYS, 2 * CTOK), f32),
                pltpu.VMEM((2, 8, 2 * CTOK), f32),
                pltpu.VMEM((8, 2 * CTOK), f32),
                pltpu.VMEM((2, 2 * CTOK, 2 * HD), bf),
                pltpu.VMEM((CHIPS * QH, HD, CTOK), bf),
                pltpu.VMEM((CHIPS * QH, 2, CTOK), f32),
                pltpu.VMEM((2, QH, HALF, CTOK), bf),
                pltpu.VMEM((2, QH, 2, CTOK), f32),
                pltpu.VMEM((2, QH, HD, CTOK), bf),
                pltpu.VMEM((2, QH, 2, CTOK), f32),
                pltpu.VMEM((QH, CTOK, HD), bf),
                pltpu.VMEM((KH, 8, CTOK), f32),
                dma((3 + 2 * LOADS,)),
                dma((2, LOADS, 2)), dma((2, LOADS, 2)),
                dma((2,)), dma((2,)),
                dma((2, KH, 2)), dma((2, KH, 2)),
                dma((KH,)), dma((KH,)),
                dma((2, KH)), dma((2, KH)),
                dma((2, KH)), dma((2, KH)),
                dma((2, KH)), dma((2, KH)),
                dma((2, KH, G)), dma((2, KH, G)),
                dma((2, KH, G)), dma((2, KH, G)),
                dma((KH,)), dma((KH,)),
                dma((2,)),
            ],
            compiler_params=pltpu.CompilerParams(
                collective_id=0, has_side_effects=True, vmem_limit_bytes=48 << 20),
        )(prefix_len, *(pltpu.with_memory_space_constraint(x, pltpu.HBM)
                        for x in (queries, key_cache, value_cache, key_new, value_new)))
        attn_out = out.transpose(1, 0, 2)
        lse = lse[:, :, :G].reshape(2 * QH, CTOK)
        row_lse = lax.dynamic_slice(lse, (0, core * TOK), (2 * QH, TOK)).T
        return attn_out, row_lse

    return jax.shard_map(local_attend, mesh=mesh, in_specs=(tok_spec, tok_spec, tok_spec, tok_spec, tok_spec, P('dp')),
                         out_specs=(tok_spec, tok_spec), check_vma=False)
```

```python
import math

import jax
import jax.numpy as jnp
from jax import lax
from jax.experimental import pallas as pl
from jax.experimental.pallas import tpu as pltpu
from jax.sharding import PartitionSpec as P

MESH = pl.DeviceIdType.MESH
NEG = -1e30
CHIPS = 4
TOK = 64
CTOK = 2 * TOK
PRE = 1536
CPRE = 2 * PRE
HD = 128
HALF = HD // 2
KVH = 8
KH = KVH // 2
G = 3
QH = KH * G
KEYS = CPRE + CTOK
TILES = KH * 6
STEP = 512
AHEAD = 8
LEAD = 3
BLK = 32
VBLK = 128
SCALE = HD ** -0.5
SCALE2 = SCALE * math.log2(math.e)
NT = (((1,), (1,)), ((), ()))
NN = (((1,), (0,)), ((), ()))
CHUNKS = [(c, STEP) for c in range(0, CPRE, STEP)] + [(CPRE, CTOK)]
LOADS = 4


def packed(digits, bits):
    return sum(d << (bits * i) for i, d in enumerate(digits))


PAIRS = [((0, 5), (1, 5)), ((0, 3), (0, 4)), ((0, 2), (1, 3)), ((1, 4), (1, 2)), ((0, 1), (0, 0)), ((1, 1), (1, 0)),
         ((2, 0), (2, 1)), ((3, 0), (3, 1)), ((2, 2), (2, 3)), ((3, 2), (3, 3)), ((2, 4), (3, 4)), ((2, 5), (3, 5))]
ORDER = [(packed([p[b][0] for p in PAIRS], 2), packed([p[b][1] % 4 for p in PAIRS], 2), packed([p[b][1] // 4 for p in PAIRS], 1))
         for b in range(2)]


def kernel(prefix_ref, q_hbm, k_hbm, v_hbm, kn_hbm, vn_hbm, out_ref, lse_ref,
           q_raw, k_raw, v_raw, kn_raw, vn_raw, qt_buf, ks_buf, vs_buf, kns_buf, vns_buf,
           q_buf, k_buf, vt_buf, vn_buf, bias_buf, fresh_buf, s0_buf, s1_buf, max_buf, top_buf, qt2_buf,
           o_buf, l_buf, t_buf, tl_buf, r_buf, rl_buf, fin_buf, finl_buf,
           in_sem, kv_send, kv_recv, n_send, n_recv, q_send, q_recv, p_send, p_recv, d_send, d_recv,
           t_send, t_recv, tl_send, tl_recv, o_send, o_recv, l_send, l_recv, f_send, f_recv, fl_sem):
    s_bufs = (s0_buf, s1_buf)
    me = lax.axis_index('cp')
    core = lax.rem(me, 2)
    chip = me // 2
    other = 1 - core

    def dev(r, c):
        return {'cp': (chip ^ r) * 2 + c}

    def remote(src, dst, send, recv, r, c):
        return pltpu.make_async_remote_copy(src, dst, send, recv, device_id=dev(r, c), device_id_type=MESH)

    part = PRE // LOADS
    loads = [pltpu.make_async_copy(q_hbm, q_raw, in_sem.at[0]),
             pltpu.make_async_copy(kn_hbm, kn_raw, in_sem.at[1]),
             pltpu.make_async_copy(vn_hbm, vn_raw, in_sem.at[2])]
    k_loads = [pltpu.make_async_copy(k_hbm.at[pl.ds(i * part, part)], k_raw.at[pl.ds(i * part, part)], in_sem.at[3 + i])
               for i in range(LOADS)]
    v_loads = [pltpu.make_async_copy(v_hbm.at[pl.ds(i * part, part)], v_raw.at[pl.ds(i * part, part)], in_sem.at[3 + LOADS + i])
               for i in range(LOADS)]
    for c in loads + k_loads + v_loads:
        c.start()

    barrier = pltpu.get_barrier_semaphore()
    peers = [dev(1, 0), dev(1, 1), dev(2, 0), dev(2, 1), dev(0, other)]
    for peer in peers:
        pl.semaphore_signal(barrier, inc=1, device_id=peer, device_id_type=MESH)

    tok_at = pl.ds(core * TOK, TOK)
    new_at = pl.ds(CPRE + core * TOK, TOK)

    def slot(r, k):
        return pl.ds(4 * G * k + G * (CHIPS - 1 - r), G)

    def q_copy(r, k, plane):
        return remote(qt_buf.at[pl.ds(plane * QH + k * G, G)], q_buf.at[slot(r, k), tok_at],
                      q_send.at[r - 1, k, plane], q_recv.at[r - 1, k, core], r, plane)

    def q_wait(r, k, s):
        remote(qt_buf.at[pl.ds(0, G)], q_buf.at[slot(r, k), pl.ds(s * TOK, TOK)],
               q_send.at[r - 1, k, s], q_recv.at[r - 1, k, s], r, s).wait_recv()

    def send_q(k):
        for plane in range(2):
            for r in (1, 2):
                q_copy(r, k, plane).start()

    def hop(i, k):
        half = pl.ds(i * TOK, TOK)
        return remote(q_buf.at[slot(1 + i, k), half], q_buf.at[slot(3, k), half], d_send.at[i, k], d_recv.at[i, k], 2 - i, core)

    def forward(k):
        for r in (1, 2):
            for s in range(2):
                q_wait(r, k, s)
        for i in range(2):
            hop(i, k).start()

    def diagonal(k):
        for i in range(2):
            hop(i, k).wait_recv()

    def part_q(k):
        return remote(qt_buf.at[pl.ds(other * QH + k * G, G)], q_buf.at[slot(0, k), tok_at], p_send.at[k], p_recv.at[k], 0, other)

    part_kn = remote(kns_buf, k_buf.at[:, new_at], n_send.at[0], n_recv.at[0], 0, other)
    part_vn = remote(vns_buf, vn_buf.at[:, tok_at], n_send.at[1], n_recv.at[1], 0, other)

    def part_k(i, two):
        heads, at = pl.ds(2 * two, 2), pl.ds(i * part, part)
        dst = pl.ds(pl.multiple_of(core * PRE + i * part, part), part)
        return remote(ks_buf.at[heads, at], k_buf.at[heads, dst], kv_send.at[0, i, two], kv_recv.at[0, i, two], 0, other)

    def part_v(i, two):
        heads, at = pl.ds(2 * two, 2), pl.ds(i * part, part)
        dst = pl.ds(pl.multiple_of(core * PRE + i * part, part), part)
        return remote(vs_buf.at[heads, :, at], vt_buf.at[heads, :, dst], kv_send.at[1, i, two], kv_recv.at[1, i, two], 0, other)

    loads[0].wait()

    @pl.loop(0, TOK // 16)
    def _(b):
        at = pl.ds(pl.multiple_of(b * 16, 16), 16)
        qt_buf[:, at, :] = jnp.swapaxes(q_raw[at], 0, 1)

    pl.semaphore_wait(barrier, len(peers))
    send_q(0)
    for k in range(KH):
        part_q(k).start()
    send_q(1)
    send_q(2)
    for c in range(2):
        @pl.when(core == c)
        def _():
            for k in range(KH):
                q_buf[slot(0, k), c * TOK:(c + 1) * TOK, :] = qt_buf[c * QH + k * G:c * QH + (k + 1) * G]

    loads[1].wait()
    for c in range(2):
        @pl.when(core == c)
        def _():
            y = jnp.swapaxes(kn_raw[...], 0, 1)
            k_buf[:, CPRE + c * TOK:CPRE + (c + 1) * TOK, :] = y[c * KH:(c + 1) * KH]
            kns_buf[...] = y[(1 - c) * KH:(2 - c) * KH]
    part_kn.start()
    for i in range(LOADS):
        k_loads[i].wait()
        for c in range(2):
            @pl.when(core == c)
            def _():
                @pl.loop(i * part // BLK, (i + 1) * part // BLK)
                def _(b):
                    at = pl.multiple_of(b * BLK, BLK)
                    y = jnp.swapaxes(k_raw[pl.ds(at, BLK)], 0, 1)
                    k_buf[:, pl.ds(c * PRE + at, BLK), :] = y[c * KH:(c + 1) * KH]
                    ks_buf[:, pl.ds(at, BLK), :] = y[(1 - c) * KH:(2 - c) * KH]
        part_k(i, 0).start()

    loads[2].wait()
    for c in range(2):
        @pl.when(core == c)
        def _():
            y = jnp.swapaxes(vn_raw[...], 0, 1)
            vn_buf[:, c * TOK:(c + 1) * TOK, :] = y[c * KH:(c + 1) * KH]
            vns_buf[...] = y[(1 - c) * KH:(2 - c) * KH]
    part_vn.start()
    for i in range(LOADS):
        v_loads[i].wait()
        for c in range(2):
            @pl.when(core == c)
            def _():
                @pl.loop(i * part // VBLK, (i + 1) * part // VBLK)
                def _(b):
                    at = pl.multiple_of(b * VBLK, VBLK)
                    y = jnp.swapaxes(v_raw[pl.ds(at, VBLK)], 0, 1)
                    for k in range(KH):
                        vt_buf[k, :, pl.ds(c * PRE + at, VBLK)] = y[c * KH + k].T
                        vs_buf[k, :, pl.ds(at, VBLK)] = y[(1 - c) * KH + k].T
        part_v(i, 0).start()

    for i in range(LOADS):
        part_k(i, 1).start()
        part_v(i, 1).start()

    row = lax.broadcasted_iota(jnp.int32, (CTOK, HD), 0)
    place = row - (lax.broadcasted_iota(jnp.int32, (CTOK, HD), 1) << 20)
    seen = prefix_ref[0] - chip * CPRE

    @pl.loop(0, CPRE // CTOK)
    def _(b):
        at = pl.multiple_of(b * CTOK, CTOK)
        bias_buf[pl.ds(at, CTOK), :] = jnp.where(place >= seen - at, NEG, 0.0).astype(jnp.bfloat16)

    bias_buf[CPRE:, :] = jnp.zeros((CTOK, HD), jnp.bfloat16)
    key_id = chip * CTOK + row
    for r in range(CHIPS):
        q_id = (chip ^ r) * CTOK + lax.broadcasted_iota(jnp.int32, (CTOK, CTOK), 1)
        mask = jnp.where(key_id <= q_id, 0.0, NEG)
        for g in range(G):
            fresh_buf[slot(r, 0).start + g] = mask

    for b in range(2):
        qt2_buf[b, :, HD:] = (lax.broadcasted_iota(jnp.int32, (2 * CTOK, HD), 1) == 0).astype(jnp.bfloat16)

    def place_of(p, b):
        kv, low, high = ORDER[b]
        k = (kv >> (2 * p)) & 3
        j = ((low >> (2 * p)) & 3) + 4 * ((high >> p) & 1)
        return k, 4 * G * k + 2 * j, 2 * j

    def load_q(n, b):
        for i in range(2):
            qt2_buf[b, i * CTOK:(i + 1) * CTOK, :HD] = q_buf[n + i]

    def fold(x, op):
        return op(x.reshape(x.shape[0] // 8, 8, 2 * CTOK), axis=0)

    def scores(k, f, b, c, top):
        at, n = CHUNKS[c]
        keys = jnp.concatenate([k_buf[k, pl.ds(at, n), :], bias_buf[pl.ds(at, n), :]], axis=1)
        s = lax.dot_general(keys, qt2_buf[b], NT, preferred_element_type=jnp.float32)
        if at == CPRE:
            s = s + jnp.concatenate([fresh_buf[f + i] for i in range(2)], axis=1)
        s_bufs[b][pl.ds(at, n), :] = s
        up = fold(s, jnp.max)
        return up if top is None else jnp.maximum(top, up)

    def values(k, b, c, ref_pt, total, acc):
        at, n = CHUNKS[c]
        p = jnp.exp2(s_bufs[b][pl.ds(at, n), :] * SCALE2 - ref_pt)
        up = fold(p, jnp.sum)
        total = up if total is None else total + up
        d = lax.dot_general(vt_buf[k, :, pl.ds(at, n)], p.astype(jnp.bfloat16), NN, preferred_element_type=jnp.float32)
        return total, (d if acc is None else acc + d)

    def advance(places, step, top):
        ahead, c = divmod(step, len(CHUNKS))
        (k, n, f), b = places[ahead], ahead % 2
        if c == 0:
            load_q(n, b)
            top = None
        top = scores(k, f, b, c, top)
        if c == len(CHUNKS) - 1:
            max_buf[b] = jnp.broadcast_to(top.max(axis=0, keepdims=True), (8, 2 * CTOK))
        return top

    def to_near(i, k):
        rows = pl.ds(k * G, G)
        return (remote(o_buf.at[slot(3, k), pl.ds(i * HALF, HALF)], t_buf.at[i, rows], t_send.at[i, k], t_recv.at[i, k], 1 + i, core),
                remote(l_buf.at[slot(3, k)], tl_buf.at[i, rows], tl_send.at[i, k], tl_recv.at[i, k], 1 + i, core))

    def to_home(r, k, g, half):
        n, h, at = pl.ds(slot(r, k).start + g, 1), pl.ds(k * G + g, 1), pl.ds(half * HALF, HALF)
        return remote(o_buf.at[n, at], r_buf.at[r - 1, h, at], o_send.at[r - 1, k, g, half], o_recv.at[r - 1, k, g, half], r, core)

    def lse_home(r, k):
        return remote(l_buf.at[slot(r, k)], rl_buf.at[r - 1, pl.ds(k * G, G)], l_send.at[r - 1, k], l_recv.at[r - 1, k], r, core)

    def plain(r, k, *gs):
        for g in gs:
            to_home(r, k, g, r - 1).start()

    def give_diagonal(k):
        for i in range(2):
            for c in to_near(i, k):
                c.start()

    def join(r, k, *gs):
        i = 2 - r
        if 0 in gs:
            for c in to_near(i, k):
                c.wait_recv()
        for g in gs:
            n, h, at = slot(r, k).start + g, k * G + g, pl.ds(i * HALF, HALF)
            la, lb = l_buf[n, 0:1, :], tl_buf[i, h, 0:1, :]
            top = jnp.maximum(la, lb)
            wa, wb = jnp.exp(la - top), jnp.exp(lb - top)
            z = wa + wb
            l_buf[n, 1:2, :] = top + jnp.log(z)
            o = (wa / z) * o_buf[n, at, :].astype(jnp.float32) + (wb / z) * t_buf[i, h].astype(jnp.float32)
            o_buf[n, at, :] = o.astype(jnp.bfloat16)
            to_home(r, k, g, i).start()
        if G - 1 in gs:
            lse_home(r, k).start()

    def rest_of_cache():
        for i in range(LOADS):
            part_k(i, 1).wait_recv()
            part_v(i, 1).wait_recv()

    def serve(p, at, *calls):
        @pl.when(p == at)
        def _():
            for fn, *args in calls:
                fn(*args)

    for k in range(KH):
        part_q(k).wait_recv()
    part_kn.wait_recv()
    for i in range(LOADS):
        part_k(i, 0).wait_recv()
    places = tuple(place_of(i // 2, i % 2) for i in range(4))
    top = None
    for step in range(AHEAD):
        top = advance(places, step, top)
    top_buf[...] = top
    part_vn.wait_recv()
    for k in range(KH):
        vt_buf[k, :, CPRE:] = vn_buf[k].T
    for i in range(LOADS):
        part_v(i, 0).wait_recv()
    forward(0)

    def pair(p, places):
        top = top_buf[...]
        step = AHEAD
        for _ in range(LEAD):
            top = advance(places, step, top)
            step += 1
        for b in range(2):
            k, n, _ = places[b]
            raw = max_buf[b, 0:1]
            ref_pt = raw * SCALE2
            total = acc = None
            for c in range(len(CHUNKS)):
                if step < AHEAD + 2 * len(CHUNKS):
                    top = advance(places, step, top)
                    step += 1
                total, acc = values(k, b, c, ref_pt, total, acc)
            total = total.sum(axis=0, keepdims=True)
            o = (acc / total).astype(jnp.bfloat16)
            lse = raw * SCALE + jnp.log(total)
            for i in range(2):
                o_buf[n + i] = o[:, i * CTOK:(i + 1) * CTOK]
                l_buf[n + i, 0:1, :] = lse[:, i * CTOK:(i + 1) * CTOK]
        top_buf[...] = top

        serve(p, 0, (forward, 1), (send_q, 3))
        serve(p, 1, (plain, 1, 0, 0, 1, 2))
        serve(p, 2, (forward, 2), (diagonal, 0), (plain, 2, 0, 1, 2))
        serve(p, 3, (forward, 3), (diagonal, 1), (plain, 1, 1, 0, 1, 2), (plain, 2, 1, 1, 2), (rest_of_cache,))
        serve(p, 4, (give_diagonal, 0), (plain, 2, 0, 0), (diagonal, 2))
        serve(p, 5, (give_diagonal, 1), (plain, 2, 1, 0), (diagonal, 3))
        serve(p, 6, (give_diagonal, 2), (join, 2, 0, 0, 1, 2), (join, 1, 0, 0, 1, 2))
        serve(p, 7, (give_diagonal, 3), (join, 2, 1, 0, 1, 2), (join, 1, 1, 0, 1, 2))
        serve(p, 8, (plain, 2, 2, 0, 1, 2), (plain, 1, 2, 0, 1), (join, 2, 2, 0, 1, 2), (join, 1, 2, 0, 1))
        serve(p, 9, (plain, 2, 3, 0, 1, 2), (plain, 1, 3, 0, 1), (join, 2, 3, 0, 1, 2), (join, 1, 3, 0, 1))
        serve(p, 10, (plain, 1, 2, 2), (plain, 1, 3, 2), (join, 1, 2, 2), (join, 1, 3, 2))
        after = jnp.minimum(p + 2, TILES // 2 - 1)
        return places[2], places[3], place_of(after, 0), place_of(after, 1)

    lax.fori_loop(0, TILES // 2, pair, places)

    part_kn.wait_send()
    part_vn.wait_send()

    @pl.loop(0, KH)
    def _(k):
        part_q(k).wait_send()
        for two in range(2):
            part_k(k, two).wait_send()
            part_v(k, two).wait_send()
        for r in (1, 2):
            for plane in range(2):
                q_copy(r, k, plane).wait_send()
        for i in range(2):
            hop(i, k).wait_send()
            for c in to_near(i, k):
                c.wait_send()

    their_at = pl.ds(other * TOK, TOK)

    def out_copy(k):
        rows = pl.ds(k * G, G)
        return remote(fin_buf.at[rows, their_at], out_ref.at[pl.ds(core * QH + k * G, G)], f_send.at[k], f_recv.at[k], 0, other)

    @pl.loop(0, KH)
    def _(k):
        for r in (1, 2):
            lse_home(r, k).wait_recv()
        for g in range(G):
            for r in (1, 2):
                for half in range(2):
                    to_home(r, k, g, half).wait_recv()
            n, h = slot(0, k).start + g, k * G + g
            own, near = l_buf[n, 0:1, :], [(rl_buf[i, h, 0:1, :], rl_buf[i, h, 1:2, :]) for i in range(2)]
            halves = []
            for half in range(2):
                ls = [own, near[0][half], near[1][1 - half]]
                top = jnp.maximum(jnp.maximum(ls[0], ls[1]), ls[2])
                ws = [jnp.exp(l - top) for l in ls]
                z = ws[0] + ws[1] + ws[2]
                if half == 0:
                    finl_buf[k, g:g + 1, :] = top + jnp.log(z)
                at = pl.ds(half * HALF, HALF)
                xs = [o_buf[n, at, :], r_buf[0, h, at, :], r_buf[1, h, at, :]]
                halves.append(sum((w / z) * x.astype(jnp.float32) for w, x in zip(ws, xs)))
            fin_buf[h] = jnp.concatenate(halves, axis=0).T.astype(jnp.bfloat16)
        out_copy(k).start()
        for g in range(G):
            out_ref[core * QH + k * G + g] = fin_buf[k * G + g, pl.ds(pl.multiple_of(core * TOK, TOK), TOK), :]

    theirs_l = remote(finl_buf, lse_ref.at[core], fl_sem.at[0], fl_sem.at[1], 0, other)
    theirs_l.start()
    lse_ref[core] = finl_buf[...]

    @pl.loop(0, KH)
    def _(k):
        for r in (1, 2):
            lse_home(r, k).wait_send()
            for g in range(G):
                for half in range(2):
                    to_home(r, k, g, half).wait_send()
        out_copy(k).wait()

    theirs_l.wait()


def solution(mesh):
    tok_spec = P(('dp', 'cp'))
    bf, f32 = jnp.bfloat16, jnp.float32
    dma = pltpu.SemaphoreType.DMA

    def local_attend(queries, key_new, value_new, key_cache, value_cache, prefix_len):
        core = lax.rem(lax.axis_index('cp'), 2)
        hbm = pl.BlockSpec(memory_space=pltpu.HBM)
        vmem = pl.BlockSpec(memory_space=pltpu.VMEM)
        out, lse = pl.pallas_call(
            kernel,
            out_shape=(pltpu.VMEM((2 * QH, TOK, HD), bf), pltpu.VMEM((2, KH, 8, CTOK), f32)),
            in_specs=[pl.BlockSpec(memory_space=pltpu.SMEM)] + [hbm] * 5,
            out_specs=(vmem, vmem),
            scratch_shapes=[
                pltpu.VMEM((TOK, 2 * QH, HD), bf),
                pltpu.VMEM((PRE, KVH, HD), bf),
                pltpu.VMEM((PRE, KVH, HD), bf),
                pltpu.VMEM((TOK, KVH, HD), bf),
                pltpu.VMEM((TOK, KVH, HD), bf),
                pltpu.VMEM((2 * QH, TOK, HD), bf),
                pltpu.VMEM((KH, PRE, HD), bf),
                pltpu.VMEM((KH, HD, PRE), bf),
                pltpu.VMEM((KH, TOK, HD), bf),
                pltpu.VMEM((KH, TOK, HD), bf),
                pltpu.VMEM((CHIPS * QH, CTOK, HD), bf),
                pltpu.VMEM((KH, KEYS, HD), bf),
                pltpu.VMEM((KH, HD, KEYS), bf),
                pltpu.VMEM((KH, CTOK, HD), bf),
                pltpu.VMEM((KEYS, HD), bf),
                pltpu.VMEM((CHIPS * G, CTOK, CTOK), f32),
                pltpu.VMEM((KEYS, 2 * CTOK), f32),
                pltpu.VMEM((KEYS, 2 * CTOK), f32),
                pltpu.VMEM((2, 8, 2 * CTOK), f32),
                pltpu.VMEM((8, 2 * CTOK), f32),
                pltpu.VMEM((2, 2 * CTOK, 2 * HD), bf),
                pltpu.VMEM((CHIPS * QH, HD, CTOK), bf),
                pltpu.VMEM((CHIPS * QH, 2, CTOK), f32),
                pltpu.VMEM((2, QH, HALF, CTOK), bf),
                pltpu.VMEM((2, QH, 2, CTOK), f32),
                pltpu.VMEM((2, QH, HD, CTOK), bf),
                pltpu.VMEM((2, QH, 2, CTOK), f32),
                pltpu.VMEM((QH, CTOK, HD), bf),
                pltpu.VMEM((KH, 8, CTOK), f32),
                dma((3 + 2 * LOADS,)),
                dma((2, LOADS, 2)), dma((2, LOADS, 2)),
                dma((2,)), dma((2,)),
                dma((2, KH, 2)), dma((2, KH, 2)),
                dma((KH,)), dma((KH,)),
                dma((2, KH)), dma((2, KH)),
                dma((2, KH)), dma((2, KH)),
                dma((2, KH)), dma((2, KH)),
                dma((2, KH, G, 2)), dma((2, KH, G, 2)),
                dma((2, KH)), dma((2, KH)),
                dma((KH,)), dma((KH,)),
                dma((2,)),
            ],
            compiler_params=pltpu.CompilerParams(
                collective_id=0, has_side_effects=True, vmem_limit_bytes=48 << 20),
        )(prefix_len, *(pltpu.with_memory_space_constraint(x, pltpu.HBM)
                        for x in (queries, key_cache, value_cache, key_new, value_new)))
        attn_out = out.transpose(1, 0, 2)
        lse = lse[:, :, :G].reshape(2 * QH, CTOK)
        row_lse = lax.dynamic_slice(lse, (0, core * TOK), (2 * QH, TOK)).T
        return attn_out, row_lse

    return jax.shard_map(local_attend, mesh=mesh, in_specs=(tok_spec, tok_spec, tok_spec, tok_spec, tok_spec, P('dp')),
                         out_specs=(tok_spec, tok_spec), check_vma=False)
```

```python
import math

import jax
import jax.numpy as jnp
from jax import lax
from jax.experimental import pallas as pl
from jax.experimental.pallas import tpu as pltpu
from jax.sharding import PartitionSpec as P

MESH = pl.DeviceIdType.MESH
NEG = -1e30
CHIPS = 4
TOK = 64
CTOK = 2 * TOK
PRE = 1536
CPRE = 2 * PRE
HD = 128
HALF = HD // 2
KVH = 8
KH = KVH // 2
G = 3
QH = KH * G
KEYS = CPRE + CTOK
TILES = KH * 6
STEP = 512
AHEAD = 8
LEAD = 3
BLK = 32
VBLK = 128
SCALE = HD ** -0.5
SCALE2 = SCALE * math.log2(math.e)
NT = (((1,), (1,)), ((), ()))
NN = (((1,), (0,)), ((), ()))
CHUNKS = [(c, STEP) for c in range(0, CPRE, STEP)] + [(CPRE, CTOK)]
LOADS = 4


def packed(digits, bits):
    return sum(d << (bits * i) for i, d in enumerate(digits))


PAIRS = [((0, 5), (1, 5)), ((0, 3), (0, 4)), ((0, 2), (1, 3)), ((1, 4), (1, 2)), ((0, 1), (0, 0)), ((1, 1), (1, 0)),
         ((2, 0), (2, 1)), ((3, 0), (3, 1)), ((2, 2), (2, 3)), ((3, 2), (3, 3)), ((2, 4), (3, 4)), ((2, 5), (3, 5))]
ORDER = [(packed([p[b][0] for p in PAIRS], 2), packed([p[b][1] % 4 for p in PAIRS], 2), packed([p[b][1] // 4 for p in PAIRS], 1))
         for b in range(2)]


def kernel(prefix_ref, q_hbm, k_hbm, v_hbm, kn_hbm, vn_hbm, out_ref, lse_ref,
           q_raw, k_raw, v_raw, kn_raw, vn_raw, qt_buf, ks_buf, vs_buf, kns_buf, vns_buf,
           q_buf, k_buf, vt_buf, vn_buf, bias_buf, fresh_buf, s0_buf, s1_buf, max_buf, top_buf, qt2_buf,
           o_buf, l_buf, t_buf, tl_buf, r_buf, rl_buf, fin_buf, finl_buf,
           in_sem, kv_send, kv_recv, n_send, n_recv, q_send, q_recv, p_send, p_recv, d_send, d_recv,
           t_send, t_recv, tl_send, tl_recv, o_send, o_recv, l_send, l_recv, f_send, f_recv, fl_sem):
    s_bufs = (s0_buf, s1_buf)
    me = lax.axis_index('cp')
    core = lax.rem(me, 2)
    chip = me // 2
    other = 1 - core

    def dev(r, c):
        return {'cp': (chip ^ r) * 2 + c}

    def remote(src, dst, send, recv, r, c):
        return pltpu.make_async_remote_copy(src, dst, send, recv, device_id=dev(r, c), device_id_type=MESH)

    part = PRE // LOADS
    loads = [pltpu.make_async_copy(q_hbm, q_raw, in_sem.at[0]),
             pltpu.make_async_copy(kn_hbm, kn_raw, in_sem.at[1]),
             pltpu.make_async_copy(vn_hbm, vn_raw, in_sem.at[2])]
    k_loads = [pltpu.make_async_copy(k_hbm.at[pl.ds(i * part, part)], k_raw.at[pl.ds(i * part, part)], in_sem.at[3 + i])
               for i in range(LOADS)]
    v_loads = [pltpu.make_async_copy(v_hbm.at[pl.ds(i * part, part)], v_raw.at[pl.ds(i * part, part)], in_sem.at[3 + LOADS + i])
               for i in range(LOADS)]
    for c in loads + k_loads + v_loads:
        c.start()

    barrier = pltpu.get_barrier_semaphore()
    peers = [dev(1, 0), dev(1, 1), dev(2, 0), dev(2, 1), dev(0, other)]
    for peer in peers:
        pl.semaphore_signal(barrier, inc=1, device_id=peer, device_id_type=MESH)

    tok_at = pl.ds(core * TOK, TOK)
    new_at = pl.ds(CPRE + core * TOK, TOK)

    def slot(r, k):
        return pl.ds(4 * G * k + G * (CHIPS - 1 - r), G)

    def q_copy(r, k, plane):
        return remote(qt_buf.at[pl.ds(plane * QH + k * G, G)], q_buf.at[slot(r, k), tok_at],
                      q_send.at[r - 1, k, plane], q_recv.at[r - 1, k], r, plane)

    def q_wait(r, k):
        remote(q_buf.at[slot(r, k)], q_buf.at[slot(r, k)], q_send.at[r - 1, k, 0], q_recv.at[r - 1, k], r, core).wait_recv()

    def send_q(k):
        for plane in range(2):
            for r in (1, 2):
                q_copy(r, k, plane).start()

    def hop(i, k):
        half = pl.ds(i * TOK, TOK)
        return remote(q_buf.at[slot(1 + i, k), half], q_buf.at[slot(3, k), half], d_send.at[i, k], d_recv.at[i, k], 2 - i, core)

    def forward(k):
        for r in (1, 2):
            q_wait(r, k)
        for i in range(2):
            hop(i, k).start()

    def diagonal(k):
        for i in range(2):
            hop(i, k).wait_recv()

    def part_q(k):
        return remote(qt_buf.at[pl.ds(other * QH + k * G, G)], q_buf.at[slot(0, k), tok_at], p_send.at[k], p_recv.at[k], 0, other)

    part_kn = remote(kns_buf, k_buf.at[:, new_at], n_send.at[0], n_recv.at[0], 0, other)
    part_vn = remote(vns_buf, vn_buf.at[:, tok_at], n_send.at[1], n_recv.at[1], 0, other)

    def part_k(i, two):
        heads, at = pl.ds(2 * two, 2), pl.ds(i * part, part)
        dst = pl.ds(pl.multiple_of(core * PRE + i * part, part), part)
        return remote(ks_buf.at[heads, at], k_buf.at[heads, dst], kv_send.at[0, i, two], kv_recv.at[0, i, two], 0, other)

    def part_v(i, two):
        heads, at = pl.ds(2 * two, 2), pl.ds(i * part, part)
        dst = pl.ds(pl.multiple_of(core * PRE + i * part, part), part)
        return remote(vs_buf.at[heads, :, at], vt_buf.at[heads, :, dst], kv_send.at[1, i, two], kv_recv.at[1, i, two], 0, other)

    loads[0].wait()

    @pl.loop(0, TOK // 16)
    def _(b):
        at = pl.ds(pl.multiple_of(b * 16, 16), 16)
        qt_buf[:, at, :] = jnp.swapaxes(q_raw[at], 0, 1)

    pl.semaphore_wait(barrier, len(peers))
    send_q(0)
    for k in range(KH):
        part_q(k).start()
    send_q(1)
    send_q(2)
    for c in range(2):
        @pl.when(core == c)
        def _():
            for k in range(KH):
                q_buf[slot(0, k), c * TOK:(c + 1) * TOK, :] = qt_buf[c * QH + k * G:c * QH + (k + 1) * G]

    loads[1].wait()
    for c in range(2):
        @pl.when(core == c)
        def _():
            y = jnp.swapaxes(kn_raw[...], 0, 1)
            k_buf[:, CPRE + c * TOK:CPRE + (c + 1) * TOK, :] = y[c * KH:(c + 1) * KH]
            kns_buf[...] = y[(1 - c) * KH:(2 - c) * KH]
    part_kn.start()
    for i in range(LOADS):
        k_loads[i].wait()
        for c in range(2):
            @pl.when(core == c)
            def _():
                @pl.loop(i * part // BLK, (i + 1) * part // BLK)
                def _(b):
                    at = pl.multiple_of(b * BLK, BLK)
                    y = jnp.swapaxes(k_raw[pl.ds(at, BLK)], 0, 1)
                    k_buf[:, pl.ds(c * PRE + at, BLK), :] = y[c * KH:(c + 1) * KH]
                    ks_buf[:, pl.ds(at, BLK), :] = y[(1 - c) * KH:(2 - c) * KH]
        part_k(i, 0).start()

    loads[2].wait()
    for c in range(2):
        @pl.when(core == c)
        def _():
            y = jnp.swapaxes(vn_raw[...], 0, 1)
            vn_buf[:, c * TOK:(c + 1) * TOK, :] = y[c * KH:(c + 1) * KH]
            vns_buf[...] = y[(1 - c) * KH:(2 - c) * KH]
    part_vn.start()
    for i in range(LOADS):
        v_loads[i].wait()
        for c in range(2):
            @pl.when(core == c)
            def _():
                @pl.loop(i * part // VBLK, (i + 1) * part // VBLK)
                def _(b):
                    at = pl.multiple_of(b * VBLK, VBLK)
                    y = jnp.swapaxes(v_raw[pl.ds(at, VBLK)], 0, 1)
                    for k in range(KH):
                        vt_buf[k, :, pl.ds(c * PRE + at, VBLK)] = y[c * KH + k].T
                        vs_buf[k, :, pl.ds(at, VBLK)] = y[(1 - c) * KH + k].T
        part_v(i, 0).start()

    for i in range(LOADS):
        part_k(i, 1).start()
        part_v(i, 1).start()

    row = lax.broadcasted_iota(jnp.int32, (CTOK, HD), 0)
    place = row - (lax.broadcasted_iota(jnp.int32, (CTOK, HD), 1) << 20)
    seen = prefix_ref[0] - chip * CPRE

    @pl.loop(0, CPRE // CTOK)
    def _(b):
        at = pl.multiple_of(b * CTOK, CTOK)
        bias_buf[pl.ds(at, CTOK), :] = jnp.where(place >= seen - at, NEG, 0.0).astype(jnp.bfloat16)

    bias_buf[CPRE:, :] = jnp.zeros((CTOK, HD), jnp.bfloat16)
    key_id = chip * CTOK + row
    for r in range(CHIPS):
        q_id = (chip ^ r) * CTOK + lax.broadcasted_iota(jnp.int32, (CTOK, CTOK), 1)
        mask = jnp.where(key_id <= q_id, 0.0, NEG)
        for g in range(G):
            fresh_buf[slot(r, 0).start + g] = mask

    for b in range(2):
        qt2_buf[b, :, HD:] = (lax.broadcasted_iota(jnp.int32, (2 * CTOK, HD), 1) == 0).astype(jnp.bfloat16)

    def place_of(p, b):
        kv, low, high = ORDER[b]
        k = (kv >> (2 * p)) & 3
        j = ((low >> (2 * p)) & 3) + 4 * ((high >> p) & 1)
        return k, 4 * G * k + 2 * j, 2 * j

    def load_q(n, b):
        for i in range(2):
            qt2_buf[b, i * CTOK:(i + 1) * CTOK, :HD] = q_buf[n + i]

    def fold(x, op):
        return op(x.reshape(x.shape[0] // 8, 8, 2 * CTOK), axis=0)

    def scores(k, f, b, c, top):
        at, n = CHUNKS[c]
        keys = jnp.concatenate([k_buf[k, pl.ds(at, n), :], bias_buf[pl.ds(at, n), :]], axis=1)
        s = lax.dot_general(keys, qt2_buf[b], NT, preferred_element_type=jnp.float32)
        if at == CPRE:
            s = s + jnp.concatenate([fresh_buf[f + i] for i in range(2)], axis=1)
        s_bufs[b][pl.ds(at, n), :] = s
        up = fold(s, jnp.max)
        return up if top is None else jnp.maximum(top, up)

    def values(k, b, c, ref_pt, total, acc):
        at, n = CHUNKS[c]
        p = jnp.exp2(s_bufs[b][pl.ds(at, n), :] * SCALE2 - ref_pt)
        up = fold(p, jnp.sum)
        total = up if total is None else total + up
        d = lax.dot_general(vt_buf[k, :, pl.ds(at, n)], p.astype(jnp.bfloat16), NN, preferred_element_type=jnp.float32)
        return total, (d if acc is None else acc + d)

    def advance(places, step, top):
        ahead, c = divmod(step, len(CHUNKS))
        (k, n, f), b = places[ahead], ahead % 2
        if c == 0:
            load_q(n, b)
            top = None
        top = scores(k, f, b, c, top)
        if c == len(CHUNKS) - 1:
            max_buf[b] = jnp.broadcast_to(top.max(axis=0, keepdims=True), (8, 2 * CTOK))
        return top

    def to_near(i, k):
        rows = pl.ds(k * G, G)
        return (remote(o_buf.at[slot(3, k), pl.ds(i * HALF, HALF)], t_buf.at[i, rows], t_send.at[i, k], t_recv.at[i, k], 1 + i, core),
                remote(l_buf.at[slot(3, k)], tl_buf.at[i, rows], tl_send.at[i, k], tl_recv.at[i, k], 1 + i, core))

    def to_home(r, k, g, half, heads=1):
        n, h, at = pl.ds(slot(r, k).start + g, heads), pl.ds(k * G + g, heads), pl.ds(half * HALF, HALF)
        return remote(o_buf.at[n, at], r_buf.at[r - 1, h, at], o_send.at[r - 1, k], o_recv.at[r - 1, k], r, core)

    def all_home(r, k):
        return remote(o_buf.at[slot(r, k)], r_buf.at[r - 1, pl.ds(k * G, G)], o_send.at[r - 1, k], o_recv.at[r - 1, k], r, core)

    def lse_home(r, k):
        return remote(l_buf.at[slot(r, k)], rl_buf.at[r - 1, pl.ds(k * G, G)], l_send.at[r - 1, k], l_recv.at[r - 1, k], r, core)

    def plain(r, k, *gs):
        to_home(r, k, gs[0], r - 1, len(gs)).start()

    def give_diagonal(k):
        for i in range(2):
            for c in to_near(i, k):
                c.start()

    def join(r, k, *gs):
        i = 2 - r
        if 0 in gs:
            for c in to_near(i, k):
                c.wait_recv()
        for g in gs:
            n, h, at = slot(r, k).start + g, k * G + g, pl.ds(i * HALF, HALF)
            la, lb = l_buf[n, 0:1, :], tl_buf[i, h, 0:1, :]
            top = jnp.maximum(la, lb)
            wa, wb = jnp.exp(la - top), jnp.exp(lb - top)
            z = wa + wb
            l_buf[n, 1:2, :] = top + jnp.log(z)
            o = (wa / z) * o_buf[n, at, :].astype(jnp.float32) + (wb / z) * t_buf[i, h].astype(jnp.float32)
            o_buf[n, at, :] = o.astype(jnp.bfloat16)
        to_home(r, k, gs[0], i, len(gs)).start()
        if G - 1 in gs:
            lse_home(r, k).start()

    def rest_of_cache():
        for i in range(LOADS):
            part_k(i, 1).wait_recv()
            part_v(i, 1).wait_recv()

    def serve(p, at, *calls):
        @pl.when(p == at)
        def _():
            for fn, *args in calls:
                fn(*args)

    for k in range(KH):
        part_q(k).wait_recv()
    part_kn.wait_recv()
    for i in range(LOADS):
        part_k(i, 0).wait_recv()
    places = tuple(place_of(i // 2, i % 2) for i in range(4))
    top = None
    for step in range(AHEAD):
        top = advance(places, step, top)
    top_buf[...] = top
    part_vn.wait_recv()
    for k in range(KH):
        vt_buf[k, :, CPRE:] = vn_buf[k].T
    for i in range(LOADS):
        part_v(i, 0).wait_recv()
    forward(0)

    def pair(p, places):
        top = top_buf[...]
        step = AHEAD
        for _ in range(LEAD):
            top = advance(places, step, top)
            step += 1
        for b in range(2):
            k, n, _ = places[b]
            raw = max_buf[b, 0:1]
            ref_pt = raw * SCALE2
            total = acc = None
            for c in range(len(CHUNKS)):
                if step < AHEAD + 2 * len(CHUNKS):
                    top = advance(places, step, top)
                    step += 1
                total, acc = values(k, b, c, ref_pt, total, acc)
            total = total.sum(axis=0, keepdims=True)
            o = (acc / total).astype(jnp.bfloat16)
            lse = raw * SCALE + jnp.log(total)
            for i in range(2):
                o_buf[n + i] = o[:, i * CTOK:(i + 1) * CTOK]
                l_buf[n + i, 0:1, :] = lse[:, i * CTOK:(i + 1) * CTOK]
        top_buf[...] = top

        serve(p, 0, (forward, 1), (send_q, 3))
        serve(p, 1, (plain, 1, 0, 0, 1, 2))
        serve(p, 2, (forward, 2), (diagonal, 0), (plain, 2, 0, 1, 2))
        serve(p, 3, (forward, 3), (diagonal, 1), (plain, 1, 1, 0, 1, 2), (plain, 2, 1, 1, 2), (rest_of_cache,))
        serve(p, 4, (give_diagonal, 0), (plain, 2, 0, 0), (diagonal, 2))
        serve(p, 5, (give_diagonal, 1), (plain, 2, 1, 0), (diagonal, 3))
        serve(p, 6, (give_diagonal, 2), (join, 2, 0, 0, 1, 2), (join, 1, 0, 0, 1, 2))
        serve(p, 7, (give_diagonal, 3), (join, 2, 1, 0, 1, 2), (join, 1, 1, 0, 1, 2))
        serve(p, 8, (plain, 2, 2, 0, 1, 2), (plain, 1, 2, 0, 1), (join, 2, 2, 0, 1, 2), (join, 1, 2, 0, 1))
        serve(p, 9, (plain, 2, 3, 0, 1, 2), (plain, 1, 3, 0, 1), (join, 2, 3, 0, 1, 2), (join, 1, 3, 0, 1))
        serve(p, 10, (plain, 1, 2, 2), (plain, 1, 3, 2), (join, 1, 2, 2), (join, 1, 3, 2))
        after = jnp.minimum(p + 2, TILES // 2 - 1)
        return places[2], places[3], place_of(after, 0), place_of(after, 1)

    lax.fori_loop(0, TILES // 2, pair, places)

    part_kn.wait_send()
    part_vn.wait_send()

    @pl.loop(0, KH)
    def _(k):
        part_q(k).wait_send()
        for two in range(2):
            part_k(k, two).wait_send()
            part_v(k, two).wait_send()
        for r in (1, 2):
            for plane in range(2):
                q_copy(r, k, plane).wait_send()
        for i in range(2):
            hop(i, k).wait_send()
            for c in to_near(i, k):
                c.wait_send()

    their_at = pl.ds(other * TOK, TOK)

    def out_copy(k):
        rows = pl.ds(k * G, G)
        return remote(fin_buf.at[rows, their_at], out_ref.at[pl.ds(core * QH + k * G, G)], f_send.at[k], f_recv.at[k], 0, other)

    @pl.loop(0, KH)
    def _(k):
        for r in (1, 2):
            lse_home(r, k).wait_recv()
            all_home(r, k).wait_recv()
        for g in range(G):
            n, h = slot(0, k).start + g, k * G + g
            own, near = l_buf[n, 0:1, :], [(rl_buf[i, h, 0:1, :], rl_buf[i, h, 1:2, :]) for i in range(2)]
            halves = []
            for half in range(2):
                ls = [own, near[0][half], near[1][1 - half]]
                top = jnp.maximum(jnp.maximum(ls[0], ls[1]), ls[2])
                ws = [jnp.exp(l - top) for l in ls]
                z = ws[0] + ws[1] + ws[2]
                if half == 0:
                    finl_buf[k, g:g + 1, :] = top + jnp.log(z)
                at = pl.ds(half * HALF, HALF)
                xs = [o_buf[n, at, :], r_buf[0, h, at, :], r_buf[1, h, at, :]]
                halves.append(sum((w / z) * x.astype(jnp.float32) for w, x in zip(ws, xs)))
            fin_buf[h] = jnp.concatenate(halves, axis=0).T.astype(jnp.bfloat16)
        out_copy(k).start()
        for g in range(G):
            out_ref[core * QH + k * G + g] = fin_buf[k * G + g, pl.ds(pl.multiple_of(core * TOK, TOK), TOK), :]

    theirs_l = remote(finl_buf, lse_ref.at[core], fl_sem.at[0], fl_sem.at[1], 0, other)
    theirs_l.start()
    lse_ref[core] = finl_buf[...]

    @pl.loop(0, KH)
    def _(k):
        for r in (1, 2):
            lse_home(r, k).wait_send()
            all_home(r, k).wait_send()
        out_copy(k).wait()

    theirs_l.wait()


def solution(mesh):
    tok_spec = P(('dp', 'cp'))
    bf, f32 = jnp.bfloat16, jnp.float32
    dma = pltpu.SemaphoreType.DMA

    def local_attend(queries, key_new, value_new, key_cache, value_cache, prefix_len):
        core = lax.rem(lax.axis_index('cp'), 2)
        hbm = pl.BlockSpec(memory_space=pltpu.HBM)
        vmem = pl.BlockSpec(memory_space=pltpu.VMEM)
        out, lse = pl.pallas_call(
            kernel,
            out_shape=(pltpu.VMEM((2 * QH, TOK, HD), bf), pltpu.VMEM((2, KH, 8, CTOK), f32)),
            in_specs=[pl.BlockSpec(memory_space=pltpu.SMEM)] + [hbm] * 5,
            out_specs=(vmem, vmem),
            scratch_shapes=[
                pltpu.VMEM((TOK, 2 * QH, HD), bf),
                pltpu.VMEM((PRE, KVH, HD), bf),
                pltpu.VMEM((PRE, KVH, HD), bf),
                pltpu.VMEM((TOK, KVH, HD), bf),
                pltpu.VMEM((TOK, KVH, HD), bf),
                pltpu.VMEM((2 * QH, TOK, HD), bf),
                pltpu.VMEM((KH, PRE, HD), bf),
                pltpu.VMEM((KH, HD, PRE), bf),
                pltpu.VMEM((KH, TOK, HD), bf),
                pltpu.VMEM((KH, TOK, HD), bf),
                pltpu.VMEM((CHIPS * QH, CTOK, HD), bf),
                pltpu.VMEM((KH, KEYS, HD), bf),
                pltpu.VMEM((KH, HD, KEYS), bf),
                pltpu.VMEM((KH, CTOK, HD), bf),
                pltpu.VMEM((KEYS, HD), bf),
                pltpu.VMEM((CHIPS * G, CTOK, CTOK), f32),
                pltpu.VMEM((KEYS, 2 * CTOK), f32),
                pltpu.VMEM((KEYS, 2 * CTOK), f32),
                pltpu.VMEM((2, 8, 2 * CTOK), f32),
                pltpu.VMEM((8, 2 * CTOK), f32),
                pltpu.VMEM((2, 2 * CTOK, 2 * HD), bf),
                pltpu.VMEM((CHIPS * QH, HD, CTOK), bf),
                pltpu.VMEM((CHIPS * QH, 2, CTOK), f32),
                pltpu.VMEM((2, QH, HALF, CTOK), bf),
                pltpu.VMEM((2, QH, 2, CTOK), f32),
                pltpu.VMEM((2, QH, HD, CTOK), bf),
                pltpu.VMEM((2, QH, 2, CTOK), f32),
                pltpu.VMEM((QH, CTOK, HD), bf),
                pltpu.VMEM((KH, 8, CTOK), f32),
                dma((3 + 2 * LOADS,)),
                dma((2, LOADS, 2)), dma((2, LOADS, 2)),
                dma((2,)), dma((2,)),
                dma((2, KH, 2)), dma((2, KH)),
                dma((KH,)), dma((KH,)),
                dma((2, KH)), dma((2, KH)),
                dma((2, KH)), dma((2, KH)),
                dma((2, KH)), dma((2, KH)),
                dma((2, KH)), dma((2, KH)),
                dma((2, KH)), dma((2, KH)),
                dma((KH,)), dma((KH,)),
                dma((2,)),
            ],
            compiler_params=pltpu.CompilerParams(
                collective_id=0, has_side_effects=True, vmem_limit_bytes=48 << 20),
        )(prefix_len, *(pltpu.with_memory_space_constraint(x, pltpu.HBM)
                        for x in (queries, key_cache, value_cache, key_new, value_new)))
        attn_out = out.transpose(1, 0, 2)
        lse = lse[:, :, :G].reshape(2 * QH, CTOK)
        row_lse = lax.dynamic_slice(lse, (0, core * TOK), (2 * QH, TOK)).T
        return attn_out, row_lse

    return jax.shard_map(local_attend, mesh=mesh, in_specs=(tok_spec, tok_spec, tok_spec, tok_spec, tok_spec, P('dp')),
                         out_specs=(tok_spec, tok_spec), check_vma=False)
```

```python
import math

import jax
import jax.numpy as jnp
from jax import lax
from jax.experimental import pallas as pl
from jax.experimental.pallas import tpu as pltpu
from jax.sharding import PartitionSpec as P

MESH = pl.DeviceIdType.MESH
NEG = -1e30
CHIPS = 4
TOK = 64
CTOK = 2 * TOK
PRE = 1536
CPRE = 2 * PRE
HD = 128
HALF = HD // 2
KVH = 8
KH = KVH // 2
G = 3
QH = KH * G
KEYS = CPRE + CTOK
TILES = KH * 6
STEP = 512
AHEAD = 8
LEAD = 3
BLK = 32
VBLK = 128
SCALE = HD ** -0.5
SCALE2 = SCALE * math.log2(math.e)
NT = (((1,), (1,)), ((), ()))
NN = (((1,), (0,)), ((), ()))
HEADS = tuple(range(G))
X, Y, FAR = range(1, CHIPS)
CHUNKS = [(c, STEP) for c in range(0, CPRE, STEP)] + [(CPRE, CTOK)]
LOADS = 4


def packed(digits, bits):
    return sum(d << (bits * i) for i, d in enumerate(digits))


PAIRS = ("051503040213", "141201001110", "202130312223", "323324342535")
TABLE = [int(d) for d in "".join(PAIRS)]
ORDER = [(packed(TABLE[2 * b::4], 2), packed([d % 4 for d in TABLE[2 * b + 1::4]], 2), packed([d // 4 for d in TABLE[2 * b + 1::4]], 1))
         for b in range(2)]


def kernel(prefix_ref, q_hbm, k_hbm, v_hbm, kn_hbm, vn_hbm, out_ref, lse_ref,
           q_raw, k_raw, v_raw, kn_raw, vn_raw, qt_buf, ks_buf, vs_buf, kns_buf, vns_buf,
           q_buf, k_buf, vt_buf, vn_buf, bias_buf, fresh_buf, s0_buf, s1_buf, max_buf, top_buf, qt2_buf,
           o_buf, l_buf, t_buf, tl_buf, r_buf, rl_buf, fin_buf, finl_buf,
           in_sem, kv_send, kv_recv, n_send, n_recv, q_send, q_recv, p_send, p_recv, d_send, d_recv,
           t_send, t_recv, tl_send, tl_recv, o_send, o_recv, l_send, l_recv, f_send, f_recv, fl_sem):
    s_bufs = (s0_buf, s1_buf)
    me = lax.axis_index('cp')
    core = lax.rem(me, 2)
    chip = me // 2
    other = 1 - core

    def dev(r, c):
        return {'cp': (chip ^ r) * 2 + c}

    def remote(src, dst, send, recv, r, c):
        return pltpu.make_async_remote_copy(src, dst, send, recv, device_id=dev(r, c), device_id_type=MESH)

    part = PRE // LOADS
    loads = [pltpu.make_async_copy(q_hbm, q_raw, in_sem.at[0]),
             pltpu.make_async_copy(kn_hbm, kn_raw, in_sem.at[1]),
             pltpu.make_async_copy(vn_hbm, vn_raw, in_sem.at[2])]
    k_loads = [pltpu.make_async_copy(k_hbm.at[pl.ds(i * part, part)], k_raw.at[pl.ds(i * part, part)], in_sem.at[3 + i])
               for i in range(LOADS)]
    v_loads = [pltpu.make_async_copy(v_hbm.at[pl.ds(i * part, part)], v_raw.at[pl.ds(i * part, part)], in_sem.at[3 + LOADS + i])
               for i in range(LOADS)]
    for c in loads + k_loads + v_loads:
        c.start()

    barrier = pltpu.get_barrier_semaphore()
    peers = [dev(1, 0), dev(1, 1), dev(2, 0), dev(2, 1), dev(0, other)]
    for peer in peers:
        pl.semaphore_signal(barrier, inc=1, device_id=peer, device_id_type=MESH)

    tok_at = pl.ds(core * TOK, TOK)
    new_at = pl.ds(CPRE + core * TOK, TOK)

    def slot(r, k):
        return pl.ds(4 * G * k + G * (CHIPS - 1 - r), G)

    def q_copy(r, k, plane):
        return remote(qt_buf.at[pl.ds(plane * QH + k * G, G)], q_buf.at[slot(r, k), tok_at],
                      q_send.at[r - 1], q_recv.at[r - 1, k], r, plane)

    def q_wait(r, k):
        remote(q_buf.at[slot(r, k)], q_buf.at[slot(r, k)], q_send.at[r - 1], q_recv.at[r - 1, k], r, core).wait_recv()

    def send_q(k):
        for plane in range(2):
            for r in (1, 2):
                q_copy(r, k, plane).start()

    def hop(i, k):
        half = pl.ds(i * TOK, TOK)
        return remote(q_buf.at[slot(1 + i, k), half], q_buf.at[slot(3, k), half], d_send.at[i], d_recv.at[i, k], 2 - i, core)

    def forward(k):
        for r in (1, 2):
            q_wait(r, k)
        for i in range(2):
            hop(i, k).start()

    def diagonal(k):
        for i in range(2):
            hop(i, k).wait_recv()

    def part_q(k):
        return remote(qt_buf.at[pl.ds(other * QH + k * G, G)], q_buf.at[slot(0, k), tok_at], p_send.at[0], p_recv.at[0], 0, other)

    part_kn = remote(kns_buf, k_buf.at[:, new_at], n_send.at[0], n_recv.at[0], 0, other)
    part_vn = remote(vns_buf, vn_buf.at[:, tok_at], n_send.at[1], n_recv.at[1], 0, other)

    def part_k(i, two):
        heads, at = pl.ds(2 * two, 2), pl.ds(i * part, part)
        dst = pl.ds(pl.multiple_of(core * PRE + i * part, part), part)
        return remote(ks_buf.at[heads, at], k_buf.at[heads, dst], kv_send.at[0], kv_recv.at[0, two], 0, other)

    def all_k(heads, two):
        dst = pl.ds(pl.multiple_of(core * PRE, PRE), PRE)
        return remote(ks_buf.at[heads], k_buf.at[heads, dst], kv_send.at[0], kv_recv.at[0, two], 0, other)

    def all_v(heads, two):
        dst = pl.ds(pl.multiple_of(core * PRE, PRE), PRE)
        return remote(vs_buf.at[heads], vt_buf.at[heads, :, dst], kv_send.at[1], kv_recv.at[1, two], 0, other)

    def part_v(i, two):
        heads, at = pl.ds(2 * two, 2), pl.ds(i * part, part)
        dst = pl.ds(pl.multiple_of(core * PRE + i * part, part), part)
        return remote(vs_buf.at[heads, :, at], vt_buf.at[heads, :, dst], kv_send.at[1], kv_recv.at[1, two], 0, other)

    loads[0].wait()

    @pl.loop(0, TOK // 16)
    def _(b):
        at = pl.ds(pl.multiple_of(b * 16, 16), 16)
        qt_buf[:, at, :] = jnp.swapaxes(q_raw[at], 0, 1)

    pl.semaphore_wait(barrier, len(peers))
    send_q(0)
    for k in range(KH):
        part_q(k).start()
    send_q(1)
    send_q(2)
    for c in range(2):
        @pl.when(core == c)
        def _():
            for k in range(KH):
                q_buf[slot(0, k), c * TOK:(c + 1) * TOK, :] = qt_buf[c * QH + k * G:c * QH + (k + 1) * G]

    loads[1].wait()
    for c in range(2):
        @pl.when(core == c)
        def _():
            y = jnp.swapaxes(kn_raw[...], 0, 1)
            k_buf[:, CPRE + c * TOK:CPRE + (c + 1) * TOK, :] = y[c * KH:(c + 1) * KH]
            kns_buf[...] = y[(1 - c) * KH:(2 - c) * KH]
    part_kn.start()
    for i in range(LOADS):
        k_loads[i].wait()
        for c in range(2):
            @pl.when(core == c)
            def _():
                @pl.loop(i * part // BLK, (i + 1) * part // BLK)
                def _(b):
                    at = pl.multiple_of(b * BLK, BLK)
                    y = jnp.swapaxes(k_raw[pl.ds(at, BLK)], 0, 1)
                    k_buf[:, pl.ds(c * PRE + at, BLK), :] = y[c * KH:(c + 1) * KH]
                    ks_buf[:, pl.ds(at, BLK), :] = y[(1 - c) * KH:(2 - c) * KH]
        part_k(i, 0).start()

    loads[2].wait()
    for c in range(2):
        @pl.when(core == c)
        def _():
            y = jnp.swapaxes(vn_raw[...], 0, 1)
            vn_buf[:, c * TOK:(c + 1) * TOK, :] = y[c * KH:(c + 1) * KH]
            vns_buf[...] = y[(1 - c) * KH:(2 - c) * KH]
    part_vn.start()
    for i in range(LOADS):
        v_loads[i].wait()
        for c in range(2):
            @pl.when(core == c)
            def _():
                @pl.loop(i * part // VBLK, (i + 1) * part // VBLK)
                def _(b):
                    at = pl.multiple_of(b * VBLK, VBLK)
                    y = jnp.swapaxes(v_raw[pl.ds(at, VBLK)], 0, 1)
                    for k in range(KH):
                        vt_buf[k, :, pl.ds(c * PRE + at, VBLK)] = y[c * KH + k].T
                        vs_buf[k, :, pl.ds(at, VBLK)] = y[(1 - c) * KH + k].T
        part_v(i, 0).start()

    for i in range(LOADS):
        part_k(i, 1).start()
        part_v(i, 1).start()

    row = lax.broadcasted_iota(jnp.int32, (CTOK, HD), 0)
    place = row - (lax.broadcasted_iota(jnp.int32, (CTOK, HD), 1) << 20)
    seen = prefix_ref[0] - chip * CPRE

    @pl.loop(0, CPRE // CTOK)
    def _(b):
        at = pl.multiple_of(b * CTOK, CTOK)
        bias_buf[pl.ds(at, CTOK), :] = jnp.where(place >= seen - at, NEG, 0.0).astype(jnp.bfloat16)

    bias_buf[CPRE:, :] = jnp.zeros((CTOK, HD), jnp.bfloat16)
    key_id = chip * CTOK + row
    for r in range(CHIPS):
        q_id = (chip ^ r) * CTOK + lax.broadcasted_iota(jnp.int32, (CTOK, CTOK), 1)
        mask = jnp.where(key_id <= q_id, 0.0, NEG)
        for g in range(G):
            fresh_buf[slot(r, 0).start + g] = mask

    for b in range(2):
        qt2_buf[b, :, HD:] = (lax.broadcasted_iota(jnp.int32, (2 * CTOK, HD), 1) == 0).astype(jnp.bfloat16)

    def place_of(p, b):
        kv, low, high = ORDER[b]
        k = (kv >> (2 * p)) & 3
        j = ((low >> (2 * p)) & 3) + 4 * ((high >> p) & 1)
        return k, 4 * G * k + 2 * j, 2 * j

    def load_q(n, b):
        for i in range(2):
            qt2_buf[b, i * CTOK:(i + 1) * CTOK, :HD] = q_buf[n + i]

    def fold(x, op):
        return op(x.reshape(x.shape[0] // 8, 8, 2 * CTOK), axis=0)

    def scores(k, f, b, c, top):
        at, n = CHUNKS[c]
        keys = jnp.concatenate([k_buf[k, pl.ds(at, n), :], bias_buf[pl.ds(at, n), :]], axis=1)
        s = lax.dot_general(keys, qt2_buf[b], NT, preferred_element_type=jnp.float32)
        if at == CPRE:
            s = s + jnp.concatenate([fresh_buf[f + i] for i in range(2)], axis=1)
        s_bufs[b][pl.ds(at, n), :] = s
        up = fold(s, jnp.max)
        return up if top is None else jnp.maximum(top, up)

    def values(k, b, c, ref_pt, total, acc):
        at, n = CHUNKS[c]
        p = jnp.exp2(s_bufs[b][pl.ds(at, n), :] * SCALE2 - ref_pt)
        up = fold(p, jnp.sum)
        total = up if total is None else total + up
        d = lax.dot_general(vt_buf[k, :, pl.ds(at, n)], p.astype(jnp.bfloat16), NN, preferred_element_type=jnp.float32)
        return total, (d if acc is None else acc + d)

    def advance(places, step, top):
        ahead, c = divmod(step, len(CHUNKS))
        (k, n, f), b = places[ahead], ahead % 2
        if c == 0:
            load_q(n, b)
            top = None
        top = scores(k, f, b, c, top)
        if c == len(CHUNKS) - 1:
            max_buf[b] = jnp.broadcast_to(top.max(axis=0, keepdims=True), (8, 2 * CTOK))
        return top

    def to_near(i, k):
        rows = pl.ds(k * G, G)
        return (remote(o_buf.at[slot(3, k), pl.ds(i * HALF, HALF)], t_buf.at[i, rows], t_send.at[i], t_recv.at[i, k], 1 + i, core),
                remote(l_buf.at[slot(3, k)], tl_buf.at[i, rows], tl_send.at[i], tl_recv.at[i, k], 1 + i, core))

    def to_home(r, k, g, half, heads=1):
        n, h, at = pl.ds(slot(r, k).start + g, heads), pl.ds(k * G + g, heads), pl.ds(half * HALF, HALF)
        return remote(o_buf.at[n, at], r_buf.at[r - 1, h, at], o_send.at[r - 1], o_recv.at[r - 1, k], r, core)

    def all_home(r, k):
        return remote(o_buf.at[slot(r, k)], r_buf.at[r - 1, pl.ds(k * G, G)], o_send.at[r - 1], o_recv.at[r - 1, k], r, core)

    def lse_home(r, k):
        return remote(l_buf.at[slot(r, k)], rl_buf.at[r - 1, pl.ds(k * G, G)], l_send.at[r - 1], l_recv.at[r - 1, k], r, core)

    def plain(r, k, *gs):
        to_home(r, k, gs[0], r - 1, len(gs)).start()

    def give_diagonal(k):
        for i in range(2):
            for c in to_near(i, k):
                c.start()

    def join(r, k, *gs):
        i = 2 - r
        if 0 in gs:
            for c in to_near(i, k):
                c.wait_recv()
        for g in gs:
            n, h, at = slot(r, k).start + g, k * G + g, pl.ds(i * HALF, HALF)
            la, lb = l_buf[n, 0:1, :], tl_buf[i, h, 0:1, :]
            top = jnp.maximum(la, lb)
            wa, wb = jnp.exp(la - top), jnp.exp(lb - top)
            z = wa + wb
            l_buf[n, 1:2, :] = top + jnp.log(z)
            o = (wa / z) * o_buf[n, at, :].astype(jnp.float32) + (wb / z) * t_buf[i, h].astype(jnp.float32)
            o_buf[n, at, :] = o.astype(jnp.bfloat16)
        to_home(r, k, gs[0], i, len(gs)).start()
        if G - 1 in gs:
            lse_home(r, k).start()

    def rest_of_cache():
        all_k(pl.ds(2, 2), 1).wait_recv()
        all_v(pl.ds(2, 2), 1).wait_recv()

    def serve(p, at, *calls):
        @pl.when(p == at)
        def _():
            for fn, *args in calls:
                fn(*args)

    all_q = remote(qt_buf.at[pl.ds(0, QH)], qt_buf.at[pl.ds(0, QH)], p_send.at[0], p_recv.at[0], 0, other)
    all_q.wait_recv()
    part_kn.wait_recv()
    all_k(pl.ds(0, 2), 0).wait_recv()
    places = tuple(place_of(i // 2, i % 2) for i in range(4))
    top = None
    for step in range(AHEAD):
        top = advance(places, step, top)
    top_buf[...] = top
    part_vn.wait_recv()
    for k in range(KH):
        vt_buf[k, :, CPRE:] = vn_buf[k].T
    all_v(pl.ds(0, 2), 0).wait_recv()
    forward(0)

    def pair(p, places):
        top = top_buf[...]
        step = AHEAD
        for _ in range(LEAD):
            top = advance(places, step, top)
            step += 1
        for b in range(2):
            k, n, _ = places[b]
            raw = max_buf[b, 0:1]
            ref_pt = raw * SCALE2
            total = acc = None
            for c in range(len(CHUNKS)):
                if step < AHEAD + 2 * len(CHUNKS):
                    top = advance(places, step, top)
                    step += 1
                total, acc = values(k, b, c, ref_pt, total, acc)
            total = total.sum(axis=0, keepdims=True)
            o = (acc / total).astype(jnp.bfloat16)
            lse = raw * SCALE + jnp.log(total)
            for i in range(2):
                o_buf[n + i] = o[:, i * CTOK:(i + 1) * CTOK]
                l_buf[n + i, 0:1, :] = lse[:, i * CTOK:(i + 1) * CTOK]
        top_buf[...] = top

        serve(p, 0, (forward, 1), (send_q, 3))
        serve(p, 1, (plain, X, 0, *HEADS))
        serve(p, 2, (forward, 2), (diagonal, 0), (plain, Y, 0, *HEADS[1:]))
        serve(p, 3, (forward, 3), (diagonal, 1), (plain, X, 1, *HEADS), (plain, Y, 1, *HEADS[1:]), (rest_of_cache,))
        serve(p, 4, (give_diagonal, 0), (plain, Y, 0, *HEADS[:1]), (diagonal, 2))
        serve(p, 5, (give_diagonal, 1), (plain, Y, 1, *HEADS[:1]), (diagonal, 3))
        serve(p, 6, (give_diagonal, 2), (join, Y, 0, *HEADS), (join, X, 0, *HEADS))
        serve(p, 7, (give_diagonal, 3), (join, Y, 1, *HEADS), (join, X, 1, *HEADS))
        for late in range(2, KH):
            serve(p, 6 + late, (plain, Y, late, *HEADS), (plain, X, late, *HEADS[:2]), (join, Y, late, *HEADS), (join, X, late, *HEADS[:2]))
        serve(p, 10, *((fn, X, late, *HEADS[2:]) for fn in (plain, join) for late in range(2, KH)))
        after = jnp.minimum(p + 2, TILES // 2 - 1)
        return places[2], places[3], place_of(after, 0), place_of(after, 1)

    lax.fori_loop(0, TILES // 2, pair, places)

    part_kn.wait_send()
    part_vn.wait_send()

    all_q.wait_send()
    all_k(pl.ds(0, KH), 0).wait_send()
    all_v(pl.ds(0, KH), 0).wait_send()
    for i in range(2):
        half = pl.ds(i * TOK, TOK)
        remote(qt_buf, qt_buf, q_send.at[i], q_recv.at[i, 0], 1 + i, core).wait_send()
        remote(q_buf.at[pl.ds(0, QH), half], q_buf.at[pl.ds(0, QH), half], d_send.at[i], d_recv.at[i, 0], 1 + i, core).wait_send()
        remote(t_buf.at[i], t_buf.at[i], t_send.at[i], t_recv.at[i, 0], 1 + i, core).wait_send()
        remote(tl_buf.at[i], tl_buf.at[i], tl_send.at[i], tl_recv.at[i, 0], 1 + i, core).wait_send()

    their_at = pl.ds(other * TOK, TOK)

    def out_copy(k):
        rows = pl.ds(k * G, G)
        return remote(fin_buf.at[rows, their_at], out_ref.at[pl.ds(core * QH + k * G, G)], f_send.at[0], f_recv.at[0], 0, other)

    @pl.loop(0, KH)
    def _(k):
        for r in (1, 2):
            lse_home(r, k).wait_recv()
            all_home(r, k).wait_recv()
        for g in range(G):
            n, h = slot(0, k).start + g, k * G + g
            own, near = l_buf[n, 0:1, :], [(rl_buf[i, h, 0:1, :], rl_buf[i, h, 1:2, :]) for i in range(2)]
            halves = []
            for half in range(2):
                ls = [own, near[0][half], near[1][1 - half]]
                top = jnp.maximum(jnp.maximum(ls[0], ls[1]), ls[2])
                ws = [jnp.exp(l - top) for l in ls]
                z = ws[0] + ws[1] + ws[2]
                if half == 0:
                    finl_buf[k, g:g + 1, :] = top + jnp.log(z)
                at = pl.ds(half * HALF, HALF)
                xs = [o_buf[n, at, :], r_buf[0, h, at, :], r_buf[1, h, at, :]]
                halves.append(sum((w / z) * x.astype(jnp.float32) for w, x in zip(ws, xs)))
            fin_buf[h] = jnp.concatenate(halves, axis=0).T.astype(jnp.bfloat16)
        out_copy(k).start()
        for g in range(G):
            out_ref[core * QH + k * G + g] = fin_buf[k * G + g, pl.ds(pl.multiple_of(core * TOK, TOK), TOK), :]

    theirs_l = remote(finl_buf, lse_ref.at[core], fl_sem.at[0], fl_sem.at[1], 0, other)
    theirs_l.start()
    lse_ref[core] = finl_buf[...]

    for i in range(2):
        remote(r_buf.at[i], r_buf.at[i], o_send.at[i], o_recv.at[i, 0], 1 + i, core).wait_send()
        remote(rl_buf.at[i], rl_buf.at[i], l_send.at[i], l_recv.at[i, 0], 1 + i, core).wait_send()
    remote(fin_buf.at[:, their_at], out_ref.at[pl.ds(core * QH, QH)], f_send.at[0], f_recv.at[0], 0, other).wait()
    theirs_l.wait()


def solution(mesh):
    tok_spec = P(('dp', 'cp'))
    bf, f32 = jnp.bfloat16, jnp.float32
    dma = pltpu.SemaphoreType.DMA

    def local_attend(queries, key_new, value_new, key_cache, value_cache, prefix_len):
        core = lax.rem(lax.axis_index('cp'), 2)
        hbm = pl.BlockSpec(memory_space=pltpu.HBM)
        vmem = pl.BlockSpec(memory_space=pltpu.VMEM)
        out, lse = pl.pallas_call(
            kernel,
            out_shape=(pltpu.VMEM((2 * QH, TOK, HD), bf), pltpu.VMEM((2, KH, 8, CTOK), f32)),
            in_specs=[pl.BlockSpec(memory_space=pltpu.SMEM)] + [hbm] * 5,
            out_specs=(vmem, vmem),
            scratch_shapes=[
                pltpu.VMEM((TOK, 2 * QH, HD), bf),
                pltpu.VMEM((PRE, KVH, HD), bf),
                pltpu.VMEM((PRE, KVH, HD), bf),
                pltpu.VMEM((TOK, KVH, HD), bf),
                pltpu.VMEM((TOK, KVH, HD), bf),
                pltpu.VMEM((2 * QH, TOK, HD), bf),
                pltpu.VMEM((KH, PRE, HD), bf),
                pltpu.VMEM((KH, HD, PRE), bf),
                pltpu.VMEM((KH, TOK, HD), bf),
                pltpu.VMEM((KH, TOK, HD), bf),
                pltpu.VMEM((CHIPS * QH, CTOK, HD), bf),
                pltpu.VMEM((KH, KEYS, HD), bf),
                pltpu.VMEM((KH, HD, KEYS), bf),
                pltpu.VMEM((KH, CTOK, HD), bf),
                pltpu.VMEM((KEYS, HD), bf),
                pltpu.VMEM((CHIPS * G, CTOK, CTOK), f32),
                pltpu.VMEM((KEYS, 2 * CTOK), f32),
                pltpu.VMEM((KEYS, 2 * CTOK), f32),
                pltpu.VMEM((2, 8, 2 * CTOK), f32),
                pltpu.VMEM((8, 2 * CTOK), f32),
                pltpu.VMEM((2, 2 * CTOK, 2 * HD), bf),
                pltpu.VMEM((CHIPS * QH, HD, CTOK), bf),
                pltpu.VMEM((CHIPS * QH, 2, CTOK), f32),
                pltpu.VMEM((2, QH, HALF, CTOK), bf),
                pltpu.VMEM((2, QH, 2, CTOK), f32),
                pltpu.VMEM((2, QH, HD, CTOK), bf),
                pltpu.VMEM((2, QH, 2, CTOK), f32),
                pltpu.VMEM((QH, CTOK, HD), bf),
                pltpu.VMEM((KH, 8, CTOK), f32),
                dma((3 + 2 * LOADS,)),
                dma((2,)), dma((2, 2)),
                dma((2,)), dma((2,)),
                dma((2,)), dma((2, KH)),
                dma((1,)), dma((1,)),
                dma((2,)), dma((2, KH)),
                dma((2,)), dma((2, KH)),
                dma((2,)), dma((2, KH)),
                dma((2,)), dma((2, KH)),
                dma((2,)), dma((2, KH)),
                dma((1,)), dma((1,)),
                dma((2,)),
            ],
            compiler_params=pltpu.CompilerParams(
                collective_id=0, has_side_effects=True, vmem_limit_bytes=48 << 20),
        )(prefix_len, *(pltpu.with_memory_space_constraint(x, pltpu.HBM)
                        for x in (queries, key_cache, value_cache, key_new, value_new)))
        attn_out = out.transpose(1, 0, 2)
        lse = lse[:, :, :G].reshape(2 * QH, CTOK)
        row_lse = lax.dynamic_slice(lse, (0, core * TOK), (2 * QH, TOK)).T
        return attn_out, row_lse

    return jax.shard_map(local_attend, mesh=mesh, in_specs=(tok_spec, tok_spec, tok_spec, tok_spec, tok_spec, P('dp')),
                         out_specs=(tok_spec, tok_spec), check_vma=False)
```

```python
import math

import jax
import jax.numpy as jnp
from jax import lax
from jax.experimental import pallas as pl
from jax.experimental.pallas import tpu as pltpu
from jax.sharding import PartitionSpec as P

MESH = pl.DeviceIdType.MESH
NEG = -1e30
CHIPS = 4
TOK = 64
CTOK = 2 * TOK
PRE = 1536
CPRE = 2 * PRE
HD = 128
HALF = HD // 2
KVH = 8
KH = KVH // 2
G = 3
QH = KH * G
KEYS = CPRE + CTOK
TILES = KH * 6
STEP = 512
AHEAD = 8
LEAD = 4
BLK = 32
VBLK = 128
SCALE = HD ** -0.5
SCALE2 = SCALE * math.log2(math.e)
NT = (((1,), (1,)), ((), ()))
NN = (((1,), (0,)), ((), ()))
HEADS = tuple(range(G))
X, Y, FAR = range(1, CHIPS)
CHUNKS = [(c, STEP) for c in range(0, CPRE, STEP)] + [(CPRE, CTOK)]
LOADS = 4


def packed(digits, bits):
    return sum(d << (bits * i) for i, d in enumerate(digits))


PAIRS = ("051503040213", "141201001110", "202130312223", "323324342535")
TABLE = [int(d) for d in "".join(PAIRS)]
ORDER = [(packed(TABLE[2 * b::4], 2), packed([d % 4 for d in TABLE[2 * b + 1::4]], 2), packed([d // 4 for d in TABLE[2 * b + 1::4]], 1))
         for b in range(2)]


def kernel(prefix_ref, q_hbm, k_hbm, v_hbm, kn_hbm, vn_hbm, out_ref, lse_ref,
           q_raw, k_raw, v_raw, kn_raw, vn_raw, qt_buf, ks_buf, vs_buf, kns_buf, vns_buf,
           q_buf, k_buf, vt_buf, vn_buf, bias_buf, fresh_buf, s0_buf, s1_buf, max_buf, top_buf, qt2_buf,
           o_buf, l_buf, t_buf, tl_buf, r_buf, rl_buf, fin_buf, finl_buf,
           in_sem, kv_send, kv_recv, n_send, n_recv, q_send, q_recv, p_send, p_recv, d_send, d_recv,
           t_send, t_recv, tl_send, tl_recv, o_send, o_recv, l_send, l_recv, f_send, f_recv, fl_sem):
    s_bufs = (s0_buf, s1_buf)
    me = lax.axis_index('cp')
    core = lax.rem(me, 2)
    chip = me // 2
    other = 1 - core

    def dev(r, c):
        return {'cp': (chip ^ r) * 2 + c}

    def remote(src, dst, send, recv, r, c):
        return pltpu.make_async_remote_copy(src, dst, send, recv, device_id=dev(r, c), device_id_type=MESH)

    part = PRE // LOADS
    loads = [pltpu.make_async_copy(q_hbm, q_raw, in_sem.at[0]),
             pltpu.make_async_copy(kn_hbm, kn_raw, in_sem.at[1]),
             pltpu.make_async_copy(vn_hbm, vn_raw, in_sem.at[2])]
    k_loads = [pltpu.make_async_copy(k_hbm.at[pl.ds(i * part, part)], k_raw.at[pl.ds(i * part, part)], in_sem.at[3 + i])
               for i in range(LOADS)]
    v_loads = [pltpu.make_async_copy(v_hbm.at[pl.ds(i * part, part)], v_raw.at[pl.ds(i * part, part)], in_sem.at[3 + LOADS + i])
               for i in range(LOADS)]
    for c in loads + k_loads + v_loads:
        c.start()

    barrier = pltpu.get_barrier_semaphore()
    peers = [dev(1, 0), dev(1, 1), dev(2, 0), dev(2, 1), dev(0, other)]
    for peer in peers:
        pl.semaphore_signal(barrier, inc=1, device_id=peer, device_id_type=MESH)

    tok_at = pl.ds(core * TOK, TOK)
    new_at = pl.ds(CPRE + core * TOK, TOK)

    def slot(r, k):
        return pl.ds(4 * G * k + G * (CHIPS - 1 - r), G)

    def q_copy(r, k, plane):
        return remote(qt_buf.at[pl.ds(plane * QH + k * G, G)], q_buf.at[slot(r, k), tok_at],
                      q_send.at[r - 1], q_recv.at[r - 1, k], r, plane)

    def q_wait(r, k):
        remote(q_buf.at[slot(r, k)], q_buf.at[slot(r, k)], q_send.at[r - 1], q_recv.at[r - 1, k], r, core).wait_recv()

    def send_q(k):
        for plane in range(2):
            for r in (1, 2):
                q_copy(r, k, plane).start()

    def hop(i, k):
        half = pl.ds(i * TOK, TOK)
        return remote(q_buf.at[slot(1 + i, k), half], q_buf.at[slot(3, k), half], d_send.at[i], d_recv.at[i, k], 2 - i, core)

    def forward(k):
        for r in (1, 2):
            q_wait(r, k)
        for i in range(2):
            hop(i, k).start()

    def diagonal(k):
        for i in range(2):
            hop(i, k).wait_recv()

    def part_q(k):
        return remote(qt_buf.at[pl.ds(other * QH + k * G, G)], q_buf.at[slot(0, k), tok_at], p_send.at[0], p_recv.at[0], 0, other)

    part_kn = remote(kns_buf, k_buf.at[:, new_at], n_send.at[0], n_recv.at[0], 0, other)
    part_vn = remote(vns_buf, vn_buf.at[:, tok_at], n_send.at[1], n_recv.at[1], 0, other)

    def part_k(i, two):
        heads, at = pl.ds(2 * two, 2), pl.ds(i * part, part)
        dst = pl.ds(pl.multiple_of(core * PRE + i * part, part), part)
        return remote(ks_buf.at[heads, at], k_buf.at[heads, dst], kv_send.at[0], kv_recv.at[0, two], 0, other)

    def all_k(heads, two):
        dst = pl.ds(pl.multiple_of(core * PRE, PRE), PRE)
        return remote(ks_buf.at[heads], k_buf.at[heads, dst], kv_send.at[0], kv_recv.at[0, two], 0, other)

    def all_v(heads, two):
        dst = pl.ds(pl.multiple_of(core * PRE, PRE), PRE)
        return remote(vs_buf.at[heads], vt_buf.at[heads, :, dst], kv_send.at[1], kv_recv.at[1, two], 0, other)

    def part_v(i, two):
        heads, at = pl.ds(2 * two, 2), pl.ds(i * part, part)
        dst = pl.ds(pl.multiple_of(core * PRE + i * part, part), part)
        return remote(vs_buf.at[heads, :, at], vt_buf.at[heads, :, dst], kv_send.at[1], kv_recv.at[1, two], 0, other)

    loads[0].wait()

    @pl.loop(0, TOK // 16)
    def _(b):
        at = pl.ds(pl.multiple_of(b * 16, 16), 16)
        qt_buf[:, at, :] = jnp.swapaxes(q_raw[at], 0, 1)

    pl.semaphore_wait(barrier, len(peers))
    send_q(0)
    for k in range(KH):
        part_q(k).start()
    send_q(1)
    send_q(2)
    for c in range(2):
        @pl.when(core == c)
        def _():
            for k in range(KH):
                q_buf[slot(0, k), c * TOK:(c + 1) * TOK, :] = qt_buf[c * QH + k * G:c * QH + (k + 1) * G]

    loads[1].wait()
    for c in range(2):
        @pl.when(core == c)
        def _():
            y = jnp.swapaxes(kn_raw[...], 0, 1)
            k_buf[:, CPRE + c * TOK:CPRE + (c + 1) * TOK, :] = y[c * KH:(c + 1) * KH]
            kns_buf[...] = y[(1 - c) * KH:(2 - c) * KH]
    part_kn.start()
    for i in range(LOADS):
        k_loads[i].wait()
        for c in range(2):
            @pl.when(core == c)
            def _():
                @pl.loop(i * part // BLK, (i + 1) * part // BLK)
                def _(b):
                    at = pl.multiple_of(b * BLK, BLK)
                    y = jnp.swapaxes(k_raw[pl.ds(at, BLK)], 0, 1)
                    k_buf[:, pl.ds(c * PRE + at, BLK), :] = y[c * KH:(c + 1) * KH]
                    ks_buf[:, pl.ds(at, BLK), :] = y[(1 - c) * KH:(2 - c) * KH]
        part_k(i, 0).start()

    loads[2].wait()
    for c in range(2):
        @pl.when(core == c)
        def _():
            y = jnp.swapaxes(vn_raw[...], 0, 1)
            vn_buf[:, c * TOK:(c + 1) * TOK, :] = y[c * KH:(c + 1) * KH]
            vns_buf[...] = y[(1 - c) * KH:(2 - c) * KH]
    part_vn.start()
    for i in range(LOADS):
        v_loads[i].wait()
        for c in range(2):
            @pl.when(core == c)
            def _():
                @pl.loop(i * part // VBLK, (i + 1) * part // VBLK)
                def _(b):
                    at = pl.multiple_of(b * VBLK, VBLK)
                    y = jnp.swapaxes(v_raw[pl.ds(at, VBLK)], 0, 1)
                    for k in range(KH):
                        vt_buf[k, :, pl.ds(c * PRE + at, VBLK)] = y[c * KH + k].T
                        vs_buf[k, :, pl.ds(at, VBLK)] = y[(1 - c) * KH + k].T
        part_v(i, 0).start()

    for i in range(LOADS):
        part_k(i, 1).start()
        part_v(i, 1).start()

    row = lax.broadcasted_iota(jnp.int32, (CTOK, HD), 0)
    place = row - (lax.broadcasted_iota(jnp.int32, (CTOK, HD), 1) << 20)
    seen = prefix_ref[0] - chip * CPRE

    @pl.loop(0, CPRE // CTOK)
    def _(b):
        at = pl.multiple_of(b * CTOK, CTOK)
        bias_buf[pl.ds(at, CTOK), :] = jnp.where(place >= seen - at, NEG, 0.0).astype(jnp.bfloat16)

    bias_buf[CPRE:, :] = jnp.zeros((CTOK, HD), jnp.bfloat16)
    key_id = chip * CTOK + row
    for r in range(CHIPS):
        q_id = (chip ^ r) * CTOK + lax.broadcasted_iota(jnp.int32, (CTOK, CTOK), 1)
        mask = jnp.where(key_id <= q_id, 0.0, NEG)
        for g in range(G):
            fresh_buf[slot(r, 0).start + g] = mask

    for b in range(2):
        qt2_buf[b, :, HD:] = (lax.broadcasted_iota(jnp.int32, (2 * CTOK, HD), 1) == 0).astype(jnp.bfloat16)

    def place_of(p, b):
        kv, low, high = ORDER[b]
        k = (kv >> (2 * p)) & 3
        j = ((low >> (2 * p)) & 3) + 4 * ((high >> p) & 1)
        return k, 4 * G * k + 2 * j, 2 * j

    def load_q(n, b):
        for i in range(2):
            qt2_buf[b, i * CTOK:(i + 1) * CTOK, :HD] = q_buf[n + i]

    def fold(x, op):
        return op(x.reshape(x.shape[0] // 8, 8, 2 * CTOK), axis=0)

    def scores(k, f, b, c, top):
        at, n = CHUNKS[c]
        keys = jnp.concatenate([k_buf[k, pl.ds(at, n), :], bias_buf[pl.ds(at, n), :]], axis=1)
        s = lax.dot_general(keys, qt2_buf[b], NT, preferred_element_type=jnp.float32)
        if at == CPRE:
            s = s + jnp.concatenate([fresh_buf[f + i] for i in range(2)], axis=1)
        s_bufs[b][pl.ds(at, n), :] = s
        up = fold(s, jnp.max)
        return up if top is None else jnp.maximum(top, up)

    def values(k, b, c, ref_pt, total, acc):
        at, n = CHUNKS[c]
        p = jnp.exp2(s_bufs[b][pl.ds(at, n), :] * SCALE2 - ref_pt)
        up = fold(p, jnp.sum)
        total = up if total is None else total + up
        d = lax.dot_general(vt_buf[k, :, pl.ds(at, n)], p.astype(jnp.bfloat16), NN, preferred_element_type=jnp.float32)
        return total, (d if acc is None else acc + d)

    def advance(places, step, top):
        ahead, c = divmod(step, len(CHUNKS))
        (k, n, f), b = places[ahead], ahead % 2
        if c == 0:
            load_q(n, b)
            top = None
        top = scores(k, f, b, c, top)
        if c == len(CHUNKS) - 1:
            max_buf[b] = jnp.broadcast_to(top.max(axis=0, keepdims=True), (8, 2 * CTOK))
        return top

    def to_near(i, k):
        rows = pl.ds(k * G, G)
        return (remote(o_buf.at[slot(3, k), pl.ds(i * HALF, HALF)], t_buf.at[i, rows], t_send.at[i], t_recv.at[i, k], 1 + i, core),
                remote(l_buf.at[slot(3, k)], tl_buf.at[i, rows], tl_send.at[i], tl_recv.at[i, k], 1 + i, core))

    def to_home(r, k, g, half, heads=1):
        n, h, at = pl.ds(slot(r, k).start + g, heads), pl.ds(k * G + g, heads), pl.ds(half * HALF, HALF)
        return remote(o_buf.at[n, at], r_buf.at[r - 1, h, at], o_send.at[r - 1], o_recv.at[r - 1, k], r, core)

    def all_home(r, k):
        return remote(o_buf.at[slot(r, k)], r_buf.at[r - 1, pl.ds(k * G, G)], o_send.at[r - 1], o_recv.at[r - 1, k], r, core)

    def lse_home(r, k):
        return remote(l_buf.at[slot(r, k)], rl_buf.at[r - 1, pl.ds(k * G, G)], l_send.at[r - 1], l_recv.at[r - 1, k], r, core)

    def plain(r, k, *gs):
        to_home(r, k, gs[0], r - 1, len(gs)).start()

    def give_diagonal(k):
        for i in range(2):
            for c in to_near(i, k):
                c.start()

    def join(r, k, *gs):
        i = 2 - r
        if 0 in gs:
            for c in to_near(i, k):
                c.wait_recv()
        for g in gs:
            n, h, at = slot(r, k).start + g, k * G + g, pl.ds(i * HALF, HALF)
            la, lb = l_buf[n, 0:1, :], tl_buf[i, h, 0:1, :]
            top = jnp.maximum(la, lb)
            wa, wb = jnp.exp(la - top), jnp.exp(lb - top)
            z = wa + wb
            l_buf[n, 1:2, :] = top + jnp.log(z)
            o = (wa / z) * o_buf[n, at, :].astype(jnp.float32) + (wb / z) * t_buf[i, h].astype(jnp.float32)
            o_buf[n, at, :] = o.astype(jnp.bfloat16)
        to_home(r, k, gs[0], i, len(gs)).start()
        if G - 1 in gs:
            lse_home(r, k).start()

    def rest_of_cache():
        all_k(pl.ds(2, 2), 1).wait_recv()
        all_v(pl.ds(2, 2), 1).wait_recv()

    def serve(p, at, *calls):
        @pl.when(p == at)
        def _():
            for fn, *args in calls:
                fn(*args)

    all_q = remote(qt_buf.at[pl.ds(0, QH)], qt_buf.at[pl.ds(0, QH)], p_send.at[0], p_recv.at[0], 0, other)
    all_q.wait_recv()
    part_kn.wait_recv()
    all_k(pl.ds(0, 2), 0).wait_recv()
    places = tuple(place_of(i // 2, i % 2) for i in range(4))
    top = None
    for step in range(AHEAD):
        top = advance(places, step, top)
    top_buf[...] = top
    part_vn.wait_recv()
    for k in range(KH):
        vt_buf[k, :, CPRE:] = vn_buf[k].T
    all_v(pl.ds(0, 2), 0).wait_recv()
    forward(0)

    def pair(p, places):
        top = top_buf[...]
        step = AHEAD
        for _ in range(LEAD):
            top = advance(places, step, top)
            step += 1
        for b in range(2):
            k, n, _ = places[b]
            raw = max_buf[b, 0:1]
            ref_pt = raw * SCALE2
            total = acc = None
            for c in range(len(CHUNKS)):
                if step < AHEAD + 2 * len(CHUNKS):
                    top = advance(places, step, top)
                    step += 1
                total, acc = values(k, b, c, ref_pt, total, acc)
            total = total.sum(axis=0, keepdims=True)
            o = (acc / total).astype(jnp.bfloat16)
            lse = raw * SCALE + jnp.log(total)
            for i in range(2):
                o_buf[n + i] = o[:, i * CTOK:(i + 1) * CTOK]
                l_buf[n + i, 0:1, :] = lse[:, i * CTOK:(i + 1) * CTOK]
        top_buf[...] = top

        serve(p, 0, (forward, 1), (send_q, 3))
        serve(p, 1, (plain, X, 0, *HEADS))
        serve(p, 2, (forward, 2), (diagonal, 0), (plain, Y, 0, *HEADS[1:]))
        serve(p, 3, (forward, 3), (diagonal, 1), (plain, X, 1, *HEADS), (plain, Y, 1, *HEADS[1:]), (rest_of_cache,))
        serve(p, 4, (give_diagonal, 0), (plain, Y, 0, *HEADS[:1]), (diagonal, 2))
        serve(p, 5, (give_diagonal, 1), (plain, Y, 1, *HEADS[:1]), (diagonal, 3))
        serve(p, 6, (give_diagonal, 2), (join, Y, 0, *HEADS), (join, X, 0, *HEADS))
        serve(p, 7, (give_diagonal, 3), (join, Y, 1, *HEADS), (join, X, 1, *HEADS))
        for late in range(2, KH):
            serve(p, 6 + late, (plain, Y, late, *HEADS), (plain, X, late, *HEADS[:2]), (join, Y, late, *HEADS), (join, X, late, *HEADS[:2]))
        serve(p, 10, *((fn, X, late, *HEADS[2:]) for fn in (plain, join) for late in range(2, KH)))
        after = jnp.minimum(p + 2, TILES // 2 - 1)
        return places[2], places[3], place_of(after, 0), place_of(after, 1)

    lax.fori_loop(0, TILES // 2, pair, places)

    part_kn.wait_send()
    part_vn.wait_send()

    all_q.wait_send()
    all_k(pl.ds(0, KH), 0).wait_send()
    all_v(pl.ds(0, KH), 0).wait_send()
    for i in range(2):
        half = pl.ds(i * TOK, TOK)
        remote(qt_buf, qt_buf, q_send.at[i], q_recv.at[i, 0], 1 + i, core).wait_send()
        remote(q_buf.at[pl.ds(0, QH), half], q_buf.at[pl.ds(0, QH), half], d_send.at[i], d_recv.at[i, 0], 1 + i, core).wait_send()
        remote(t_buf.at[i], t_buf.at[i], t_send.at[i], t_recv.at[i, 0], 1 + i, core).wait_send()
        remote(tl_buf.at[i], tl_buf.at[i], tl_send.at[i], tl_recv.at[i, 0], 1 + i, core).wait_send()

    their_at = pl.ds(other * TOK, TOK)

    def out_copy(k):
        rows = pl.ds(k * G, G)
        return remote(fin_buf.at[rows, their_at], out_ref.at[pl.ds(core * QH + k * G, G)], f_send.at[0], f_recv.at[0], 0, other)

    @pl.loop(0, KH)
    def _(k):
        for r in (1, 2):
            lse_home(r, k).wait_recv()
            all_home(r, k).wait_recv()
        for g in range(G):
            n, h = slot(0, k).start + g, k * G + g
            own, near = l_buf[n, 0:1, :], [(rl_buf[i, h, 0:1, :], rl_buf[i, h, 1:2, :]) for i in range(2)]
            halves = []
            for half in range(2):
                ls = [own, near[0][half], near[1][1 - half]]
                top = jnp.maximum(jnp.maximum(ls[0], ls[1]), ls[2])
                ws = [jnp.exp(l - top) for l in ls]
                z = ws[0] + ws[1] + ws[2]
                if half == 0:
                    finl_buf[k, g:g + 1, :] = top + jnp.log(z)
                at = pl.ds(half * HALF, HALF)
                xs = [o_buf[n, at, :], r_buf[0, h, at, :], r_buf[1, h, at, :]]
                halves.append(sum((w / z) * x.astype(jnp.float32) for w, x in zip(ws, xs)))
            fin_buf[h] = jnp.concatenate(halves, axis=0).T.astype(jnp.bfloat16)
        out_copy(k).start()
        for g in range(G):
            out_ref[core * QH + k * G + g] = fin_buf[k * G + g, pl.ds(pl.multiple_of(core * TOK, TOK), TOK), :]

    theirs_l = remote(finl_buf, lse_ref.at[core], fl_sem.at[0], fl_sem.at[1], 0, other)
    theirs_l.start()
    lse_ref[core] = finl_buf[...]

    for i in range(2):
        remote(r_buf.at[i], r_buf.at[i], o_send.at[i], o_recv.at[i, 0], 1 + i, core).wait_send()
        remote(rl_buf.at[i], rl_buf.at[i], l_send.at[i], l_recv.at[i, 0], 1 + i, core).wait_send()
    remote(fin_buf.at[:, their_at], out_ref.at[pl.ds(core * QH, QH)], f_send.at[0], f_recv.at[0], 0, other).wait()
    theirs_l.wait()


def solution(mesh):
    tok_spec = P(('dp', 'cp'))
    bf, f32 = jnp.bfloat16, jnp.float32
    dma = pltpu.SemaphoreType.DMA

    def local_attend(queries, key_new, value_new, key_cache, value_cache, prefix_len):
        core = lax.rem(lax.axis_index('cp'), 2)
        hbm = pl.BlockSpec(memory_space=pltpu.HBM)
        vmem = pl.BlockSpec(memory_space=pltpu.VMEM)
        out, lse = pl.pallas_call(
            kernel,
            out_shape=(pltpu.VMEM((2 * QH, TOK, HD), bf), pltpu.VMEM((2, KH, 8, CTOK), f32)),
            in_specs=[pl.BlockSpec(memory_space=pltpu.SMEM)] + [hbm] * 5,
            out_specs=(vmem, vmem),
            scratch_shapes=[
                pltpu.VMEM((TOK, 2 * QH, HD), bf),
                pltpu.VMEM((PRE, KVH, HD), bf),
                pltpu.VMEM((PRE, KVH, HD), bf),
                pltpu.VMEM((TOK, KVH, HD), bf),
                pltpu.VMEM((TOK, KVH, HD), bf),
                pltpu.VMEM((2 * QH, TOK, HD), bf),
                pltpu.VMEM((KH, PRE, HD), bf),
                pltpu.VMEM((KH, HD, PRE), bf),
                pltpu.VMEM((KH, TOK, HD), bf),
                pltpu.VMEM((KH, TOK, HD), bf),
                pltpu.VMEM((CHIPS * QH, CTOK, HD), bf),
                pltpu.VMEM((KH, KEYS, HD), bf),
                pltpu.VMEM((KH, HD, KEYS), bf),
                pltpu.VMEM((KH, CTOK, HD), bf),
                pltpu.VMEM((KEYS, HD), bf),
                pltpu.VMEM((CHIPS * G, CTOK, CTOK), f32),
                pltpu.VMEM((KEYS, 2 * CTOK), f32),
                pltpu.VMEM((KEYS, 2 * CTOK), f32),
                pltpu.VMEM((2, 8, 2 * CTOK), f32),
                pltpu.VMEM((8, 2 * CTOK), f32),
                pltpu.VMEM((2, 2 * CTOK, 2 * HD), bf),
                pltpu.VMEM((CHIPS * QH, HD, CTOK), bf),
                pltpu.VMEM((CHIPS * QH, 2, CTOK), f32),
                pltpu.VMEM((2, QH, HALF, CTOK), bf),
                pltpu.VMEM((2, QH, 2, CTOK), f32),
                pltpu.VMEM((2, QH, HD, CTOK), bf),
                pltpu.VMEM((2, QH, 2, CTOK), f32),
                pltpu.VMEM((QH, CTOK, HD), bf),
                pltpu.VMEM((KH, 8, CTOK), f32),
                dma((3 + 2 * LOADS,)),
                dma((2,)), dma((2, 2)),
                dma((2,)), dma((2,)),
                dma((2,)), dma((2, KH)),
                dma((1,)), dma((1,)),
                dma((2,)), dma((2, KH)),
                dma((2,)), dma((2, KH)),
                dma((2,)), dma((2, KH)),
                dma((2,)), dma((2, KH)),
                dma((2,)), dma((2, KH)),
                dma((1,)), dma((1,)),
                dma((2,)),
            ],
            compiler_params=pltpu.CompilerParams(
                collective_id=0, has_side_effects=True, vmem_limit_bytes=48 << 20),
        )(prefix_len, *(pltpu.with_memory_space_constraint(x, pltpu.HBM)
                        for x in (queries, key_cache, value_cache, key_new, value_new)))
        attn_out = out.transpose(1, 0, 2)
        lse = lse[:, :, :G].reshape(2 * QH, CTOK)
        row_lse = lax.dynamic_slice(lse, (0, core * TOK), (2 * QH, TOK)).T
        return attn_out, row_lse

    return jax.shard_map(local_attend, mesh=mesh, in_specs=(tok_spec, tok_spec, tok_spec, tok_spec, tok_spec, P('dp')),
                         out_specs=(tok_spec, tok_spec), check_vma=False)
```
